256 devices in a mesh: seq: 32 (over z, y), batch: 8 (over x, core).
Axes of the slice: x: 4, y: 4, z: 8, core: 2. Of those that a mesh axis runs over, the one named last changes fastest.
Arguments:
- inputs: bfloat16 [65536, 4096], P(('batch', 'seq')), parts along dimension 0, may hold values from -6 to 6
- recur_weight: bfloat16 [16, 256, 256], replicated, may hold values from -0.375 to 0.375
- input_weight: bfloat16 [16, 256, 256], replicated, may hold values from -0.375 to 0.375
- recur_bias: float32 [4096], replicated, may hold values from -4 to 4
- input_bias: float32 [4096], replicated, may hold values from -4 to 4
- decay_rate: float32 [4096], replicated, may hold values from 1.2207031e-06 to 0.02
- kv_weight: bfloat16 [4096, 512], replicated, may hold values from -61 to 61
Outputs:
- attended: bfloat16 [65536, 4096], P(('batch', 'seq')), parts along dimension 0
The draws below stay inside these ranges and needn't reach their ends.
There are 8 independent parts, one for each index of `batch`. The reference program is written for one: setup_inputs(seed, part) draws one part's arguments, and reference() takes and returns one part's arrays. A program takes and returns all parts, laid end to end along the dimension named above; an argument that names none is the same for every part. Nothing has to cross between parts.
All inputs are finite; a program needn't handle non-finite values.
Results may differ from the reference program's by a relative error of at most 0.03.
Values may be sent and summed in bfloat16 or wider, within the bound.
A program may use at most 128 MiB of HBM per device.

```python
import math
import jax
import jax.numpy as jnp
from jax import lax

D = 4096
HEAD_DIM = 256
BLOCKS = 16
BLOCK_WIDTH = 256
WINDOW = 2048
TOK_DEV = 256
SEQ_LEN = 8192


def draw_kv_weight(key, part):
    first, second = jax.random.split(jax.random.fold_in(key, 7331))
    heads = D // HEAD_DIM
    base = jax.random.normal(first, (D, 2 * HEAD_DIM), jnp.float32) * D ** (-0.5)
    base = jnp.clip(base, -6.0 * D ** (-0.5), 6.0 * D ** (-0.5))
    level = jax.random.uniform(second, (heads,), jnp.float32)
    lowest = 2.0 / HEAD_DIM ** 0.5
    highest = 24.0 / HEAD_DIM ** 0.5
    strength = jnp.exp(jnp.log(lowest) + level * (jnp.log(highest) - jnp.log(lowest)))
    identity = jnp.eye(HEAD_DIM, dtype=jnp.float32)
    aligned = (strength[:, None, None] * identity[None, :, :]).reshape(D, HEAD_DIM)
    key_cols = base[:, :HEAD_DIM] + aligned
    return jnp.concatenate([key_cols, base[:, HEAD_DIM:]], axis=1).astype(jnp.bfloat16)


def shard_levels(rng, shape, cuts, low, top_value):
    def one(dim, blocks):
        steps = jax.random.uniform(jax.random.fold_in(jax.random.fold_in(rng, 6), dim), (blocks,), jnp.float32, low / len(cuts), top_value / len(cuts))
        return jnp.repeat(jnp.exp(steps), shape[dim] // blocks).reshape((-1,) + (1,) * (len(shape) - dim - 1))

    loudness = one(*cuts[0])
    for cut in cuts[1:]:
        loudness = loudness * one(*cut)
    return loudness


def noise(own_key, dims, deviation, limit, shards=(), kind=jnp.bfloat16):
    level = shard_levels(own_key, dims, shards, -0.22, 0.18) if shards else 1.0
    values = jax.random.normal(own_key, dims, jnp.float32) * deviation * level
    return jnp.minimum(jnp.maximum(values, -limit), limit).astype(kind)


def setup_inputs(seed: int = 0, part: int = 0) -> dict:
    streams_of = jax.random.split(jax.random.key(seed), 8)
    part_splits = jax.random.split(jax.random.fold_in(streams_of[7], part), 8)
    return {
        "inputs": noise(part_splits[0], (SEQ_LEN, D), 1.0, 6.0, ((0, 32),)),
        "recur_weight": noise(streams_of[1], (BLOCKS, BLOCK_WIDTH, BLOCK_WIDTH), BLOCK_WIDTH ** -0.5, 0.375),
        "input_weight": noise(streams_of[2], (BLOCKS, BLOCK_WIDTH, BLOCK_WIDTH), BLOCK_WIDTH ** -0.5, 0.375),
        "recur_bias": noise(streams_of[3], (D,), 1.0, 4.0, (), jnp.float32),
        "input_bias": noise(streams_of[4], (D,), 1.0, 4.0, (), jnp.float32),
        "decay_rate": jnp.clip(jnp.exp(jax.random.uniform(streams_of[5], (D,), jnp.float32, math.log(1.220703097715159e-06), math.log(0.02))), 1.220703097715159e-06, 0.02),
        "kv_weight": draw_kv_weight(jax.random.fold_in(streams_of[7], 71), part),
    }


def combine_steps(earlier, later):
    return (earlier[0] * later[0], later[0] * earlier[1] + later[1])

def block_gate(inputs, weight, bias):
    total_rows = inputs.shape[0]
    split = inputs.astype(jnp.float32).reshape(total_rows, weight.shape[0], weight.shape[1])
    mixed = jnp.einsum('tbi,bio->tbo', split, weight.astype(jnp.float32))
    return jax.nn.sigmoid(mixed.reshape(total_rows, -1) + bias)

def reference(inputs, recur_weight, input_weight, recur_bias, input_bias, decay_rate, kv_weight):
    total_rows = inputs.shape[0]
    width_all = inputs.shape[1]
    recurrence = block_gate(inputs, recur_weight, recur_bias)
    input_gate = block_gate(inputs, input_weight, input_bias)
    decay_step = jnp.exp(-8.0 * recurrence * decay_rate)
    driven = jnp.sqrt(1.0 - decay_step * decay_step) * (input_gate * inputs.astype(jnp.float32))
    cumulative, state = lax.associative_scan(combine_steps, (decay_step, driven), axis=0)
    hidden = state.astype(jnp.bfloat16)
    keyval = jnp.dot(hidden, kv_weight, preferred_element_type=jnp.float32).astype(jnp.bfloat16)
    head_dim = kv_weight.shape[1] // 2
    heads = width_all // head_dim
    reach = (WINDOW + TOK_DEV - 2) // TOK_DEV
    padded = jnp.concatenate([jnp.zeros((reach * TOK_DEV, 2 * head_dim), jnp.bfloat16), keyval], axis=0)
    scale = head_dim ** (-0.5)

    def block_out(index):
        start = (index * TOK_DEV).astype(jnp.int32)
        local_kv = lax.dynamic_slice_in_dim(padded, start, (reach + 1) * TOK_DEV, 0).astype(jnp.float32)
        queries = lax.dynamic_slice_in_dim(hidden, start, TOK_DEV, 0).astype(jnp.float32)
        queries = queries.reshape(TOK_DEV, heads, head_dim).transpose(1, 0, 2)
        keys = local_kv[:, :head_dim]
        values = local_kv[:, head_dim:]
        query_pos = start + jnp.arange(TOK_DEV, dtype=jnp.int32)
        key_pos = start - reach * TOK_DEV + jnp.arange((reach + 1) * TOK_DEV, dtype=jnp.int32)
        allowed = (key_pos[None, :] <= query_pos[:, None]) & (key_pos[None, :] > query_pos[:, None] - WINDOW) & (key_pos[None, :] >= 0)
        scores = jnp.einsum('htd,kd->htk', queries, keys) * scale
        scores = jnp.where(allowed[None], scores, -1e+30)
        highest = lax.optimization_barrier(jnp.max(scores, axis=-1, keepdims=True))
        expo = jnp.exp(scores - highest)
        weights = (expo / lax.optimization_barrier(jnp.sum(expo, axis=-1, keepdims=True))).astype(jnp.bfloat16)
        result = jnp.einsum('htk,kd->htd', weights.astype(jnp.float32), values).astype(jnp.bfloat16)
        return result.transpose(1, 0, 2).reshape(TOK_DEV, width_all)
    blocks_out = lax.map(block_out, jnp.arange(total_rows // TOK_DEV, dtype=jnp.int32))
    return blocks_out.reshape(total_rows, width_all)
```

```python
import functools
import math

import jax
import jax.numpy as jnp
from jax import lax
from jax.experimental import pallas as pl
from jax.experimental.pallas import tpu as pltpu
from jax.sharding import PartitionSpec as P

TOK = 256
D = 4096
HD = 256
HEADS = 16
REACH = 8
SEQ = 32
SCALE2 = (HD ** -0.5) * math.log2(math.e)
LOG2E = math.log2(math.e)
NEG = -1e30


def token_of(row):
    return (row % 8) * 32 + row // 8


def permutation(transposed):
    rows = lax.broadcasted_iota(jnp.int32, (TOK, TOK), 1 if transposed else 0)
    toks = lax.broadcasted_iota(jnp.int32, (TOK, TOK), 0 if transposed else 1)
    return (token_of(rows) == toks).astype(jnp.bfloat16)


def causal_mask():
    q = token_of(lax.broadcasted_iota(jnp.int32, (TOK, TOK), 0))
    k = token_of(lax.broadcasted_iota(jnp.int32, (TOK, TOK), 1))
    return k <= q


def scan_block(perm, x, wr, wi, br, bi, rate, loc_ref, cum_ref):
    xp = jnp.dot(perm, x, preferred_element_type=jnp.float32)
    xb = xp.astype(jnp.bfloat16)
    lr = jnp.dot(xb, wr, preferred_element_type=jnp.float32)
    li = jnp.dot(xb, wi, preferred_element_type=jnp.float32)
    tr = jnp.tanh(lr * 0.5 + br * 0.5)
    ti = jnp.tanh(li * 0.5 + bi * 0.5)
    coef = rate * (-4.0 * LOG2E)
    a = jnp.exp2(tr * coef + coef)
    v = jnp.maximum(1.0 - a * a, 1e-37)
    drv = (v * lax.rsqrt(v)) * ((ti * 0.5 + 0.5) * xp)
    h = drv[0:8]
    c = a[0:8]
    loc_ref[0:8, :] = h
    cum_ref[0:8, :] = c
    for j in range(1, 32):
        aj = a[8 * j : 8 * j + 8]
        h = aj * h + drv[8 * j : 8 * j + 8]
        c = c * aj
        loc_ref[8 * j : 8 * j + 8, :] = h
        cum_ref[8 * j : 8 * j + 8, :] = c
    width = x.shape[1]
    carry = jnp.zeros((1, width), jnp.float32)
    prod = jnp.ones((1, width), jnp.float32)
    carries, prods = [], []
    for s in range(8):
        carries.append(carry)
        prods.append(prod)
        carry = c[s : s + 1] * carry + h[s : s + 1]
        prod = prod * c[s : s + 1]
    return (
        jnp.concatenate(carries, axis=0),
        jnp.concatenate(prods, axis=0),
        carry,
        prod,
    )


def scan_kernel(x_ref, wr_ref, wi_ref, br_ref, bi_ref, rate_ref,
                loc_ref, cum_ref, segc_ref, segp_ref, tot_ref, perm_ref):
    @pl.when(pl.program_id(0) == 0)
    def _():
        perm_ref[...] = permutation(False)

    segc, segp, carry, prod = scan_block(
        perm_ref[...], x_ref[...], wr_ref[0], wi_ref[0], br_ref[...], bi_ref[...],
        rate_ref[...], loc_ref, cum_ref,
    )
    segc_ref[...] = segc
    segp_ref[...] = segp
    tot_ref[...] = jnp.concatenate([prod, carry], axis=0)


def local_scan(x, wr, wi, br, bi, rate):
    row = lambda b: (0, b)
    f32 = jnp.float32
    return pl.pallas_call(
        scan_kernel,
        grid=(HEADS,),
        in_specs=[
            pl.BlockSpec((TOK, HD), row),
            pl.BlockSpec((1, HD, HD), lambda b: (b, 0, 0)),
            pl.BlockSpec((1, HD, HD), lambda b: (b, 0, 0)),
            pl.BlockSpec((1, HD), row),
            pl.BlockSpec((1, HD), row),
            pl.BlockSpec((1, HD), row),
        ],
        out_specs=[
            pl.BlockSpec((TOK, HD), row),
            pl.BlockSpec((TOK, HD), row),
            pl.BlockSpec((8, HD), row),
            pl.BlockSpec((8, HD), row),
            pl.BlockSpec((2, HD), row),
        ],
        out_shape=[
            jax.ShapeDtypeStruct((TOK, D), f32),
            jax.ShapeDtypeStruct((TOK, D), f32),
            jax.ShapeDtypeStruct((8, D), f32),
            jax.ShapeDtypeStruct((8, D), f32),
            jax.ShapeDtypeStruct((2, D), f32),
        ],
        scratch_shapes=[pltpu.VMEM((TOK, TOK), jnp.bfloat16)],
        cost_estimate=pl.CostEstimate(flops=1_600_000_000, bytes_accessed=16_000_000, transcendentals=0),
        name="local_scan",
    )(x, wr, wi, br[None], bi[None], rate[None])


def hidden_block(loc, cum, g):
    n = loc.shape[1]
    return (loc.reshape(32, 8, n) + cum.reshape(32, 8, n) * g[None]).reshape(TOK, n).astype(jnp.bfloat16)


def kv_kernel(loc_ref, cum_ref, segc_ref, segp_ref, carry_ref, w_ref, hid_ref, kv_ref, acc_ref):
    step = pl.program_id(0)
    g = segc_ref[...] + segp_ref[...] * carry_ref[...]
    hid = hidden_block(loc_ref[...], cum_ref[...], g)
    hid_ref[...] = hid
    part = jnp.dot(hid, w_ref[...], preferred_element_type=jnp.float32)

    @pl.when(step == 0)
    def _():
        acc_ref[...] = part

    @pl.when(step > 0)
    def _():
        acc_ref[...] += part

    @pl.when(step == pl.num_programs(0) - 1)
    def _():
        kv_ref[...] = acc_ref[...].astype(jnp.bfloat16)


def hidden_and_kv(loc, cum, segc, segp, carry, w):
    ch = 1024
    row = lambda b: (0, b)
    return pl.pallas_call(
        kv_kernel,
        grid=(D // ch,),
        in_specs=[
            pl.BlockSpec((TOK, ch), row),
            pl.BlockSpec((TOK, ch), row),
            pl.BlockSpec((8, ch), row),
            pl.BlockSpec((8, ch), row),
            pl.BlockSpec((1, ch), row),
            pl.BlockSpec((ch, 2 * HD), lambda b: (b, 0)),
        ],
        out_specs=[pl.BlockSpec((TOK, ch), row), pl.BlockSpec((TOK, 2 * HD), lambda b: (0, 0))],
        out_shape=[
            jax.ShapeDtypeStruct((TOK, D), jnp.bfloat16),
            jax.ShapeDtypeStruct((TOK, 2 * HD), jnp.bfloat16),
        ],
        scratch_shapes=[pltpu.VMEM((TOK, 2 * HD), jnp.float32)],
        name="hidden_kv",
    )(loc, cum, segc, segp, carry, w)


def attend_head(h, hid_ref, kv, mask, first, m_ref, l_ref, acc_ref):
    cols = pl.ds(pl.multiple_of(h * HD, HD), HD)
    q = hid_ref[:, cols]
    s = lax.dot_general(q, kv[:, :HD], (((1,), (1,)), ((), ())), preferred_element_type=jnp.float32)
    if mask is not None:
        s = jnp.where(mask, s, NEG)
    top = jnp.broadcast_to(jnp.max(s, axis=1, keepdims=True), (TOK, 128))
    if not first:
        before = m_ref[h]
        top = jnp.maximum(before, top)
        alpha = jnp.exp2((before - top) * SCALE2)
    m_ref[h] = top
    shift = top * SCALE2
    p = jnp.exp2(s * SCALE2 - jnp.concatenate([shift] * (s.shape[1] // 128), axis=1))
    part = sum(p[:, 128 * k : 128 * k + 128] for k in range(s.shape[1] // 128))
    out = jnp.dot(p.astype(jnp.bfloat16), kv[:, HD:], preferred_element_type=jnp.float32)
    if first:
        l_ref[h] = part
        acc_ref[:, cols] = out
    else:
        l_ref[h] = l_ref[h] * alpha + part
        acc_ref[:, cols] = acc_ref[:, cols] * jnp.concatenate([alpha, alpha], axis=1) + out


def finish_head(h, back, l_ref, acc_ref, out_ref):
    cols = pl.ds(pl.multiple_of(h * HD, HD), HD)
    total = jnp.sum(l_ref[h], axis=1, keepdims=True)
    o = (acc_ref[:, cols] * (1.0 / total)).astype(jnp.bfloat16)
    out_ref[:, cols] = jnp.dot(back, o, preferred_element_type=jnp.float32).astype(jnp.bfloat16)


UNROLL = 4


def over_heads(fn):
    def body(i, _):
        for u in range(UNROLL):
            fn(i * UNROLL + u)
        return 0

    lax.fori_loop(0, HEADS // UNROLL, body, 0)


def attend_kernel(hid_ref, kv_ref, out_ref, m_ref, l_ref, acc_ref):
    me = lax.axis_index("seq")
    mask = causal_mask()
    over_heads(lambda h: attend_head(h, hid_ref, kv_ref.at[0], mask, True, m_ref, l_ref, acc_ref))
    for o in range(1, REACH + 1):
        @pl.when(me >= o)
        def _():
            other = ~causal_mask() if o == REACH else None
            over_heads(lambda h: attend_head(h, hid_ref, kv_ref.at[o], other, False, m_ref, l_ref, acc_ref))

    back = permutation(True)
    over_heads(lambda h: finish_head(h, back, l_ref, acc_ref, out_ref))


def attention(hid, kv_all):
    vmem = pl.BlockSpec(memory_space=pltpu.VMEM)
    return pl.pallas_call(
        attend_kernel,
        in_specs=[vmem, vmem],
        out_specs=vmem,
        out_shape=jax.ShapeDtypeStruct((TOK, D), jnp.bfloat16),
        scratch_shapes=[
            pltpu.VMEM((HEADS, TOK, 128), jnp.float32),
            pltpu.VMEM((HEADS, TOK, 128), jnp.float32),
            pltpu.VMEM((TOK, D), jnp.float32),
        ],
        compiler_params=pltpu.CompilerParams(vmem_limit_bytes=48 * 1024 * 1024),
        name="attend",
    )(hid, kv_all)


def entering_state(totals):
    both = lax.all_to_all(
        jnp.broadcast_to(totals[None], (SEQ, *totals.shape)), "seq", 0, 0, tiled=True
    )
    me = lax.axis_index("seq")
    carry = jnp.zeros((D,), jnp.float32)
    for i in range(SEQ - 1):
        carry = jnp.where(i < me, both[i, 0] * carry + both[i, 1], carry)
    return carry[None]


def shifted(block, distance):
    route = [(i - distance, i) for i in range(distance, SEQ)]
    return lax.ppermute(block, "seq", route)


def on_device(inputs, recur_weight, input_weight, recur_bias, input_bias, decay_rate, kv_weight):
    loc, cum, segc, segp, tot = local_scan(
        inputs, recur_weight, input_weight, recur_bias, input_bias, decay_rate
    )
    carry = entering_state(tot)
    hid, kv = hidden_and_kv(loc, cum, segc, segp, carry, kv_weight)
    kv_all = jnp.stack([kv] + [shifted(kv, o) for o in range(1, REACH + 1)])
    return attention(hid, kv_all)


def solution(mesh):
    placed = (P(("batch", "seq"), None), P(), P(), P(), P(), P(), P())
    return jax.shard_map(
        on_device, mesh=mesh, in_specs=placed, out_specs=P(("batch", "seq"), None), check_vma=False
    )
```

```python
import math

import jax
import jax.numpy as jnp
from jax import lax
from jax.experimental import pallas as pl
from jax.experimental.pallas import tpu as pltpu
from jax.sharding import PartitionSpec as P

TOK = 256
D = 4096
HD = 256
HEADS = 16
ROWS = 8
COLS = 4
CHUNKS = 4
PER = HEADS // CHUNKS
LOG2E = math.log2(math.e)
SCALE2 = (HD ** -0.5) * LOG2E
NEG = -1e30
F32 = jnp.float32
BF16 = jnp.bfloat16
MESH = pl.DeviceIdType.MESH

STEPS = ((4,), (1, 3), (8, 5), (2, 7), (6,))
PLACE = {0: 0}
for _step in STEPS:
    for _o in _step:
        PLACE[_o] = len(PLACE)


def token_of(row):
    return (row % 8) * 32 + row // 8


def permutation(transposed):
    rows = lax.broadcasted_iota(jnp.int32, (TOK, TOK), 1 if transposed else 0)
    toks = lax.broadcasted_iota(jnp.int32, (TOK, TOK), 0 if transposed else 1)
    return (token_of(rows) == toks).astype(F32).astype(BF16)


def row_distance(o, y):
    return (o - y + COLS - 1) // COLS


class Halo:
    def __init__(self, kv, send, recv, z, y):
        self.kv, self.send, self.recv, self.z, self.y = kv, send, recv, z, y
        self.count = [0] * COLS
        self.waited = [set() for _ in range(COLS)]
        self.started = [[] for _ in range(COLS)]

    def half(self, o, part):
        return self.kv.at[PLACE[o], pl.ds(part * HD, HD)]

    def copy(self, index, src, dst, part, dz, dst_y):
        return pltpu.make_async_remote_copy(
            src_ref=self.half(src, part),
            dst_ref=self.half(dst, part),
            send_sem=self.send.at[index],
            recv_sem=self.recv.at[PLACE[dst], part],
            device_id={"seq": (self.z + dz) * COLS + dst_y},
            device_id_type=MESH,
        )

    def start(self, yy, src, part, dz, dst_y):
        dst = src + dz * COLS + dst_y - yy
        low = row_distance(src, yy)
        high = ROWS - 2 if dz else ROWS - 1
        index = self.count[yy]
        self.count[yy] += 1
        args = (index, src, dst, part, dz, dst_y)

        @pl.when((self.z >= low) & (self.z <= high))
        def _():
            self.copy(*args).start()

        self.started[yy].append((low, high, args))

    def arrive(self, yy, o, part):
        if (o, part) in self.waited[yy]:
            return
        self.waited[yy].add((o, part))

        @pl.when(self.z >= row_distance(o, yy))
        def _():
            pltpu.make_async_remote_copy(
                src_ref=self.half(o, part),
                dst_ref=self.half(o, part),
                send_sem=self.send.at[0],
                recv_sem=self.recv.at[PLACE[o], part],
                device_id={"seq": self.z * COLS + self.y},
                device_id_type=MESH,
            ).wait_recv()

    def each(self, fn):
        for yy in range(COLS):
            @pl.when(self.y == yy)
            def _():
                fn(yy)

    def own(self, yy):
        for part in (0, 1):
            self.start(yy, 0, part, 1, yy)
            if yy < COLS - 1:
                self.start(yy, 0, part, 0, yy + 1)
            if yy == 0:
                self.start(yy, 0, part, 0, COLS - 1)

    def first_row(self, yy):
        for part in (0, 1):
            self.arrive(yy, 4, part)
            self.start(yy, 4, part, 1, yy)
            self.start(yy, 4, part, 0, (yy + 1) % COLS)
            self.start(yy, 4, part, 0, (yy - 1) % COLS)
            if yy == 1 and part == 0:
                self.arrive(yy, 1, 0)
                self.start(yy, 1, 0, 0, 2)
            if yy == 2:
                self.arrive(yy, 1, part)
                self.start(yy, 1, part, 0, 3)
            if yy == 3 and part == 1:
                self.arrive(yy, 3, 1)
                self.start(yy, 3, 1, 0, 2)

    def second_row(self, yy):
        left, right = (yy - 1) % COLS, (yy + 1) % COLS
        from_left, from_right = 4 + yy - left, 4 + yy - right
        self.arrive(yy, from_left, 0)
        self.start(yy, from_left, 0, 0, right)
        for part in (0, 1):
            self.arrive(yy, 8, part)
            if yy >= 1:
                self.start(yy, 8, part, 0, yy - 1)
            if yy == COLS - 1:
                self.start(yy, 8, part, 0, 0)
        self.arrive(yy, from_right, 1)
        self.start(yy, from_right, 1, 0, left)

    def last_row(self, yy):
        if yy == 0:
            self.arrive(yy, 5, 1)
            self.start(yy, 5, 1, 0, 1)
        if yy == 1:
            for part in (0, 1):
                self.arrive(yy, 7, part)
                self.start(yy, 7, part, 0, 0)
        if yy == 2:
            self.arrive(yy, 7, 0)
            self.start(yy, 7, 0, 0, 1)

    def need(self, step):
        def fn(yy):
            for o in step:
                for part in (0, 1):
                    self.arrive(yy, o, part)

        self.each(fn)

    def drain(self):
        def fn(yy):
            for low, high, args in self.started[yy]:
                @pl.when((self.z >= low) & (self.z <= high))
                def _(args=args):
                    self.copy(*args).wait_send()

        self.each(fn)


def kernel(
    x_hbm, wr_hbm, wi_hbm, br, bi, rate, wkv_hbm, out_hbm,
    x, wr, wi, wkv, perm, xp_a, lr_a, li_a, xp_b, lr_b, li_b, loc, cum, segc, segp,
    rowtot, rowpre, coltot, carry, hid, kvacc, kv, bias0, bias8,
    m, l, acc, s_a, s_b, p_a, p_b, al_a, al_b, out,
    load_sem, row_send, row_recv, col_send, col_recv, halo_send, halo_recv, out_sem,
):
    me = lax.axis_index("seq")
    z, y = me // COLS, me % COLS

    loads = []
    for c in range(CHUNKS):
        cols, blocks = pl.ds(c * PER * HD, PER * HD), pl.ds(c * PER, PER)
        loads.append([
            pltpu.make_async_copy(x_hbm.at[:, cols], x.at[:, cols], load_sem.at[3 * c]),
            pltpu.make_async_copy(wr_hbm.at[blocks], wr.at[blocks], load_sem.at[3 * c + 1]),
            pltpu.make_async_copy(wi_hbm.at[blocks], wi.at[blocks], load_sem.at[3 * c + 2]),
        ])
    load_kv = pltpu.make_async_copy(wkv_hbm, wkv, load_sem.at[3 * CHUNKS])
    for group in loads:
        for load in group:
            load.start()
    load_kv.start()

    barrier = pltpu.get_barrier_semaphore()
    for k in range(1, COLS):
        pl.semaphore_signal(
            barrier, inc=1, device_id={"seq": z * COLS + (y + k) % COLS}, device_id_type=MESH
        )
    for k in range(1, ROWS):
        pl.semaphore_signal(
            barrier, inc=1, device_id={"seq": ((z + k) % ROWS) * COLS + y}, device_id_type=MESH
        )

    perm[...] = permutation(False)
    kt = token_of(lax.broadcasted_iota(jnp.int32, (TOK, TOK), 0))
    qt = token_of(lax.broadcasted_iota(jnp.int32, (TOK, TOK), 1))
    bias0[...] = jnp.where(kt <= qt, 0.0, NEG)
    bias8[...] = jnp.where(kt <= qt, NEG, 0.0)

    def lanes(b):
        return pl.ds(pl.multiple_of(b * HD, HD), HD)

    def gates(b, xp_ref, lr_ref, li_ref):
        xp = jnp.dot(perm[...], x[:, lanes(b)], preferred_element_type=F32)
        xb = xp.astype(BF16)
        xp_ref[...] = xp
        lr_ref[...] = jnp.dot(xb, wr[b], preferred_element_type=F32)
        li_ref[...] = jnp.dot(xb, wi[b], preferred_element_type=F32)

    def scan(b, c, xp_ref, lr_ref, li_ref):
        half_r, half_i = br[:, lanes(b)] * 0.5, bi[:, lanes(b)] * 0.5
        coef = rate[:, lanes(b)] * (-4.0 * LOG2E)
        for j in range(32):
            rows = slice(8 * j, 8 * j + 8)
            tr = jnp.tanh(lr_ref[rows] * 0.5 + half_r)
            ti = jnp.tanh(li_ref[rows] * 0.5 + half_i)
            a = jnp.exp2(tr * coef + coef)
            v = jnp.maximum(1.0 - a * a, 1e-37)
            drive = (v * lax.rsqrt(v)) * ((ti * 0.5 + 0.5) * xp_ref[rows])
            if j == 0:
                h, prod = drive, a
            else:
                h, prod = a * h + drive, prod * a
            loc[b, rows] = h
            cum[b, rows] = prod
        start = jnp.zeros((1, HD), F32)
        gain = jnp.ones((1, HD), F32)
        starts, gains = [], []
        for s in range(8):
            starts.append(start)
            gains.append(gain)
            start = prod[s : s + 1] * start + h[s : s + 1]
            gain = gain * prod[s : s + 1]
        segc[b] = jnp.concatenate(starts, axis=0)
        segp[b] = jnp.concatenate(gains, axis=0)
        rowtot[c, y, 0, b - c * PER] = gain
        rowtot[c, y, 1, b - c * PER] = start

    def row_copy(c, k):
        return pltpu.make_async_remote_copy(
            src_ref=rowtot.at[c, y], dst_ref=rowtot.at[c, y],
            send_sem=row_send.at[c, k - 1], recv_sem=row_recv.at[c, y],
            device_id={"seq": z * COLS + (y + k) % COLS}, device_id_type=MESH,
        )

    def row_arrival(c, src):
        return pltpu.make_async_remote_copy(
            src_ref=rowtot.at[c, src], dst_ref=rowtot.at[c, src],
            send_sem=row_send.at[c, 0], recv_sem=row_recv.at[c, src],
            device_id={"seq": me}, device_id_type=MESH,
        )

    def col_copy(c, to):
        return pltpu.make_async_remote_copy(
            src_ref=coltot.at[c, z], dst_ref=coltot.at[c, z],
            send_sem=col_send.at[c, to], recv_sem=col_recv.at[c, z],
            device_id={"seq": to * COLS + y}, device_id_type=MESH,
        )

    def col_arrival(c, src):
        return pltpu.make_async_remote_copy(
            src_ref=coltot.at[c, src], dst_ref=coltot.at[c, src],
            send_sem=col_send.at[c, 0], recv_sem=col_recv.at[c, src],
            device_id={"seq": me}, device_id_type=MESH,
        )

    def send_row(c):
        for k in range(1, COLS):
            row_copy(c, k).start()

    def row_totals(c):
        for k in range(1, COLS):
            row_arrival(c, (y + k) % COLS).wait_recv()
        prod, state = rowtot[c, 0, 0], rowtot[c, 0, 1]
        before_p, before_s = jnp.ones_like(prod), jnp.zeros_like(state)
        for s in range(1, COLS):
            here = s <= y
            before_p = jnp.where(here, prod, before_p)
            before_s = jnp.where(here, state, before_s)
            prod, state = prod * rowtot[c, s, 0], rowtot[c, s, 0] * state + rowtot[c, s, 1]
        rowpre[c, 0] = before_p
        rowpre[c, 1] = before_s
        coltot[c, z, 0] = prod
        coltot[c, z, 1] = state
        for to in range(1, ROWS):
            @pl.when(to > z)
            def _():
                col_copy(c, to).start()

    def hidden(c):
        carry[...] = jnp.zeros(carry.shape, F32)
        for src in range(ROWS - 1):
            @pl.when(src < z)
            def _():
                col_arrival(c, src).wait_recv()
                carry[...] = coltot[c, src, 0] * carry[...] + coltot[c, src, 1]
        carry[...] = rowpre[c, 0] * carry[...] + rowpre[c, 1]
        total = None
        for i in range(PER):
            b = c * PER + i
            g = segc[b] + segp[b] * carry[i]
            value = loc[b].reshape(32, 8, HD) + cum[b].reshape(32, 8, HD) * g[None]
            value = value.reshape(TOK, HD).astype(BF16)
            hid[b] = value
            part = jnp.dot(value, wkv[b], preferred_element_type=F32)
            total = part if total is None else total + part
        if c == 0:
            kvacc[...] = total
        else:
            kvacc[...] += total

    for load in loads[0]:
        load.wait()
    gates(0, xp_a, lr_a, li_a)
    for c in range(CHUNKS):
        if c + 1 < CHUNKS:
            for load in loads[c + 1]:
                load.wait()

        def pair(i, _, c=c):
            b = c * PER + 2 * i
            gates(b + 1, xp_b, lr_b, li_b)
            scan(b, c, xp_a, lr_a, li_a)
            gates(jnp.minimum(b + 2, HEADS - 1), xp_a, lr_a, li_a)
            scan(b + 1, c, xp_b, lr_b, li_b)
            return 0

        lax.fori_loop(0, PER // 2, pair, 0)
        if c == 0:
            pl.semaphore_wait(barrier, COLS + ROWS - 2)
        send_row(c)
        if c >= 1:
            row_totals(c - 1)
    load_kv.wait()
    for c in range(CHUNKS - 1):
        hidden(c)
        if c == 0:
            row_totals(CHUNKS - 1)
    hidden(CHUNKS - 1)
    kv[0, :HD] = kvacc[:, :HD].astype(BF16)
    kv[0, HD:] = kvacc[:, HD:].T.astype(BF16)

    halo = Halo(kv, halo_send, halo_recv, z, y)
    halo.each(halo.own)

    def attend(offsets):
        place, n = PLACE[offsets[0]], len(offsets)
        nk = n * HD
        first = offsets[0] == 0

        def qk(h, s):
            keys = kv[place : place + n, :HD].reshape(nk, HD)
            s[:nk] = lax.dot_general(
                keys, hid[h], (((1,), (1,)), ((), ())), preferred_element_type=F32
            )

        def soft(h, s, p, al):
            value = s[:nk]
            bias = bias0 if first else bias8 if offsets[0] == 8 else None
            if bias is not None:
                masked = value[:HD] + bias[...]
                value = masked if n == 1 else jnp.concatenate([masked, value[HD:]], axis=0)
            top = jnp.max(value, axis=0, keepdims=True)
            if not first:
                before = m[h]
                top = jnp.maximum(before, top)
                alpha = jnp.exp2((before - top) * SCALE2)
                al[...] = alpha
            m[h] = top
            e = jnp.exp2(value * SCALE2 - top * SCALE2)
            part = jnp.sum(e, axis=0, keepdims=True)
            l[h] = part if first else l[h] * alpha + part
            p[:nk] = e.astype(BF16)

        def pv(h, p, al):
            new = jnp.dot(kv[place, HD:], p[:HD], preferred_element_type=F32)
            if n == 2:
                new += jnp.dot(kv[place + 1, HD:], p[HD:], preferred_element_type=F32)
            acc[h] = new if first else acc[h] * al[...] + new

        qk(0, s_a)
        qk(1, s_b)
        soft(0, s_a, p_a, al_a)

        def body(i, _):
            h = 2 * i + 1
            qk(h + 1, s_a)
            pv(h - 1, p_a, al_a)
            soft(h, s_b, p_b, al_b)
            qk(h + 2, s_b)
            pv(h, p_b, al_b)
            soft(h + 1, s_a, p_a, al_a)
            return 0

        lax.fori_loop(0, HEADS // 2 - 1, body, 0)
        pv(HEADS - 2, p_a, al_a)
        soft(HEADS - 1, s_b, p_b, al_b)
        pv(HEADS - 1, p_b, al_b)

    attend((0,))
    halo.each(halo.first_row)
    for index, step in enumerate(STEPS):
        halo.need(step)

        @pl.when(me >= max(step))
        def _():
            attend(step)

        if len(step) == 2:
            @pl.when((me >= min(step)) & (me < max(step)))
            def _():
                attend((min(step),))

        if index == 0:
            halo.each(halo.second_row)
        if index == 1:
            halo.each(halo.last_row)

    back = permutation(True)
    perm[...] = back

    def finish(i, _):
        for u in range(2):
            h = 2 * i + u
            o = (acc[h] * (1.0 / l[h])).astype(BF16)
            out[:, lanes(h)] = lax.dot_general(
                perm[...], o, (((1,), (1,)), ((), ())), preferred_element_type=F32
            ).astype(BF16)
        return 0

    stores = []
    for c in range(CHUNKS):
        lax.fori_loop(c * PER // 2, (c + 1) * PER // 2, finish, 0)
        cols = pl.ds(c * PER * HD, PER * HD)
        store = pltpu.make_async_copy(out.at[:, cols], out_hbm.at[:, cols], out_sem.at[c])
        store.start()
        stores.append(store)

    halo.drain()
    for c in range(CHUNKS):
        for k in range(1, COLS):
            row_copy(c, k).wait_send()
        for to in range(1, ROWS):
            @pl.when(to > z)
            def _():
                col_copy(c, to).wait_send()
    for store in stores:
        store.wait()


def on_device(inputs, recur_weight, input_weight, recur_bias, input_bias, decay_rate, kv_weight):
    hbm = pl.BlockSpec(memory_space=pl.ANY)
    vmem = pl.BlockSpec(memory_space=pltpu.VMEM)
    tile = pltpu.VMEM((TOK, HD), F32)
    dma = pltpu.SemaphoreType.DMA
    return pl.pallas_call(
        kernel,
        in_specs=[hbm, hbm, hbm, vmem, vmem, vmem, hbm],
        out_specs=hbm,
        out_shape=jax.ShapeDtypeStruct((TOK, D), BF16),
        scratch_shapes=[
            pltpu.VMEM((TOK, D), BF16),
            pltpu.VMEM((HEADS, HD, HD), BF16),
            pltpu.VMEM((HEADS, HD, HD), BF16),
            pltpu.VMEM((HEADS, HD, 2 * HD), BF16),
            pltpu.VMEM((TOK, TOK), BF16),
            tile, tile, tile, tile, tile, tile,
            pltpu.VMEM((HEADS, TOK, HD), F32),
            pltpu.VMEM((HEADS, TOK, HD), F32),
            pltpu.VMEM((HEADS, 8, HD), F32),
            pltpu.VMEM((HEADS, 8, HD), F32),
            pltpu.VMEM((CHUNKS, COLS, 2, PER, 1, HD), F32),
            pltpu.VMEM((CHUNKS, 2, PER, 1, HD), F32),
            pltpu.VMEM((CHUNKS, ROWS, 2, PER, 1, HD), F32),
            pltpu.VMEM((PER, 1, HD), F32),
            pltpu.VMEM((HEADS, TOK, HD), BF16),
            pltpu.VMEM((TOK, 2 * HD), F32),
            pltpu.VMEM((9, 2 * HD, HD), BF16),
            tile, tile,
            pltpu.VMEM((HEADS, 1, TOK), F32),
            pltpu.VMEM((HEADS, 1, TOK), F32),
            pltpu.VMEM((HEADS, HD, TOK), F32),
            pltpu.VMEM((2 * HD, TOK), F32),
            pltpu.VMEM((2 * HD, TOK), F32),
            pltpu.VMEM((2 * HD, TOK), BF16),
            pltpu.VMEM((2 * HD, TOK), BF16),
            pltpu.VMEM((1, TOK), F32),
            pltpu.VMEM((1, TOK), F32),
            pltpu.VMEM((TOK, D), BF16),
            dma((3 * CHUNKS + 1,)),
            dma((CHUNKS, COLS - 1)),
            dma((CHUNKS, COLS)),
            dma((CHUNKS, ROWS)),
            dma((CHUNKS, ROWS)),
            dma((24,)),
            dma((9, 2)),
            dma((CHUNKS,)),
        ],
        compiler_params=pltpu.CompilerParams(
            collective_id=0, has_side_effects=True, vmem_limit_bytes=56 * 1024 * 1024
        ),
        name="layer",
    )(
        inputs, recur_weight, input_weight, recur_bias[None], input_bias[None],
        decay_rate[None], kv_weight.reshape(HEADS, HD, 2 * HD),
    )


def solution(mesh):
    placed = (P(("batch", "seq"), None), P(), P(), P(), P(), P(), P())
    return jax.shard_map(
        on_device, mesh=mesh, in_specs=placed, out_specs=P(("batch", "seq"), None), check_vma=False
    )
```

```python
import math

import jax
import jax.numpy as jnp
from jax import lax
from jax.experimental import pallas as pl
from jax.experimental.pallas import tpu as pltpu
from jax.sharding import PartitionSpec as P

TOK = 256
D = 4096
HD = 256
HEADS = 16
ROWS = 8
COLS = 4
CHUNKS = 4
PER = HEADS // CHUNKS
LOG2E = math.log2(math.e)
SCALE2 = (HD ** -0.5) * LOG2E
NEG = -1e30
F32 = jnp.float32
BF16 = jnp.bfloat16
MESH = pl.DeviceIdType.MESH

STEPS = ((4,), (1, 3), (8, 5), (2, 7), (6,))
PLACE = {0: 0}
for _step in STEPS:
    for _o in _step:
        PLACE[_o] = len(PLACE)


def token_of(row):
    return (row % 8) * 32 + row // 8


def permutation(transposed):
    rows = lax.broadcasted_iota(jnp.int32, (TOK, TOK), 1 if transposed else 0)
    toks = lax.broadcasted_iota(jnp.int32, (TOK, TOK), 0 if transposed else 1)
    return (token_of(rows) == toks).astype(F32).astype(BF16)


def row_distance(o, y):
    return (o - y + COLS - 1) // COLS


class Halo:
    def __init__(self, kv, send, recv, z, y):
        self.kv, self.send, self.recv, self.z, self.y = kv, send, recv, z, y
        self.count = [0] * COLS
        self.waited = [set() for _ in range(COLS)]
        self.started = [[] for _ in range(COLS)]

    def half(self, o, part):
        return self.kv.at[PLACE[o], pl.ds(part * HD, HD)]

    def copy(self, index, src, dst, part, dz, dst_y):
        return pltpu.make_async_remote_copy(
            src_ref=self.half(src, part),
            dst_ref=self.half(dst, part),
            send_sem=self.send.at[index],
            recv_sem=self.recv.at[PLACE[dst], part],
            device_id={"seq": (self.z + dz) * COLS + dst_y},
            device_id_type=MESH,
        )

    def start(self, yy, src, part, dz, dst_y):
        dst = src + dz * COLS + dst_y - yy
        low = row_distance(src, yy)
        high = ROWS - 2 if dz else ROWS - 1
        index = self.count[yy]
        self.count[yy] += 1
        args = (index, src, dst, part, dz, dst_y)

        @pl.when((self.z >= low) & (self.z <= high))
        def _():
            self.copy(*args).start()

        self.started[yy].append((low, high, args))

    def arrive(self, yy, o, part):
        if (o, part) in self.waited[yy]:
            return
        self.waited[yy].add((o, part))

        @pl.when(self.z >= row_distance(o, yy))
        def _():
            pltpu.make_async_remote_copy(
                src_ref=self.half(o, part),
                dst_ref=self.half(o, part),
                send_sem=self.send.at[0],
                recv_sem=self.recv.at[PLACE[o], part],
                device_id={"seq": self.z * COLS + self.y},
                device_id_type=MESH,
            ).wait_recv()

    def each(self, fn):
        for yy in range(COLS):
            @pl.when(self.y == yy)
            def _():
                fn(yy)

    def own(self, yy):
        for part in (0, 1):
            self.start(yy, 0, part, 1, yy)
            if yy < COLS - 1:
                self.start(yy, 0, part, 0, yy + 1)
            if yy == 0:
                self.start(yy, 0, part, 0, COLS - 1)

    def first_row(self, yy):
        for part in (0, 1):
            self.arrive(yy, 4, part)
            self.start(yy, 4, part, 1, yy)
            self.start(yy, 4, part, 0, (yy + 1) % COLS)
            self.start(yy, 4, part, 0, (yy - 1) % COLS)
            if yy == 1 and part == 0:
                self.arrive(yy, 1, 0)
                self.start(yy, 1, 0, 0, 2)
            if yy == 2:
                self.arrive(yy, 1, part)
                self.start(yy, 1, part, 0, 3)
            if yy == 3 and part == 1:
                self.arrive(yy, 3, 1)
                self.start(yy, 3, 1, 0, 2)

    def second_row(self, yy):
        left, right = (yy - 1) % COLS, (yy + 1) % COLS
        from_left, from_right = 4 + yy - left, 4 + yy - right
        self.arrive(yy, from_left, 0)
        self.start(yy, from_left, 0, 0, right)
        for part in (0, 1):
            self.arrive(yy, 8, part)
            if yy >= 1:
                self.start(yy, 8, part, 0, yy - 1)
            if yy == COLS - 1:
                self.start(yy, 8, part, 0, 0)
        self.arrive(yy, from_right, 1)
        self.start(yy, from_right, 1, 0, left)

    def last_row(self, yy):
        if yy == 0:
            self.arrive(yy, 5, 1)
            self.start(yy, 5, 1, 0, 1)
        if yy == 1:
            for part in (0, 1):
                self.arrive(yy, 7, part)
                self.start(yy, 7, part, 0, 0)
        if yy == 2:
            self.arrive(yy, 7, 0)
            self.start(yy, 7, 0, 0, 1)

    def need(self, step):
        def fn(yy):
            for o in step:
                for part in (0, 1):
                    self.arrive(yy, o, part)

        self.each(fn)

    def drain(self):
        def fn(yy):
            for low, high, args in self.started[yy]:
                @pl.when((self.z >= low) & (self.z <= high))
                def _(args=args):
                    self.copy(*args).wait_send()

        self.each(fn)


def kernel(
    x_hbm, wr_hbm, wi_hbm, br_hbm, bi_hbm, rate_hbm, wkv_hbm, out,
    x, wr, wi, br, bi, rate, wkv, perm, xp_a, lr_a, li_a, xp_b, lr_b, li_b, loc, cum, segc, segp,
    rowtot, rowpre, coltot, carry, hid, kvacc, kv, bias0, bias8,
    m, l, acc, s_a, s_b, p_a, p_b, al_a, al_b,
    load_sem, row_send, row_recv, col_send, col_recv, halo_send, halo_recv,
):
    me = lax.axis_index("seq")
    z, y = me // COLS, me % COLS

    loads = []
    for c in range(CHUNKS):
        cols, blocks = pl.ds(c * PER * HD, PER * HD), pl.ds(c * PER, PER)
        loads.append([
            pltpu.make_async_copy(x_hbm.at[:, cols], x.at[:, cols], load_sem.at[3 * c]),
            pltpu.make_async_copy(wr_hbm.at[blocks], wr.at[blocks], load_sem.at[3 * c + 1]),
            pltpu.make_async_copy(wi_hbm.at[blocks], wi.at[blocks], load_sem.at[3 * c + 2]),
        ])
    load_kv = pltpu.make_async_copy(wkv_hbm, wkv, load_sem.at[3 * CHUNKS])
    small = [
        pltpu.make_async_copy(src, dst, load_sem.at[3 * CHUNKS + 1 + k])
        for k, (src, dst) in enumerate([(br_hbm, br), (bi_hbm, bi), (rate_hbm, rate)])
    ]
    loads[0] += small
    for group in loads:
        for load in group:
            load.start()
    load_kv.start()

    barrier = pltpu.get_barrier_semaphore()
    for k in range(1, COLS):
        pl.semaphore_signal(
            barrier, inc=1, device_id={"seq": z * COLS + (y + k) % COLS}, device_id_type=MESH
        )
    for k in range(1, ROWS):
        pl.semaphore_signal(
            barrier, inc=1, device_id={"seq": ((z + k) % ROWS) * COLS + y}, device_id_type=MESH
        )

    perm[...] = permutation(False)
    kt = token_of(lax.broadcasted_iota(jnp.int32, (TOK, TOK), 1))
    qt = token_of(lax.broadcasted_iota(jnp.int32, (TOK, TOK), 0))
    bias0[...] = jnp.where(kt <= qt, 0.0, NEG)
    bias8[...] = jnp.where(kt <= qt, NEG, 0.0)

    def lanes(b):
        return pl.ds(pl.multiple_of(b * HD, HD), HD)

    def gates(b, xp_ref, lr_ref, li_ref):
        xp = jnp.dot(perm[...], x[:, lanes(b)], preferred_element_type=F32)
        xb = xp.astype(BF16)
        xp_ref[...] = xp
        lr_ref[...] = jnp.dot(xb, wr[b], preferred_element_type=F32)
        li_ref[...] = jnp.dot(xb, wi[b], preferred_element_type=F32)

    def scan(b, c, xp_ref, lr_ref, li_ref):
        half_r, half_i = br[:, lanes(b)] * 0.5, bi[:, lanes(b)] * 0.5
        coef = rate[:, lanes(b)] * (-4.0 * LOG2E)
        for j in range(32):
            rows = slice(8 * j, 8 * j + 8)
            tr = jnp.tanh(lr_ref[rows] * 0.5 + half_r)
            ti = jnp.tanh(li_ref[rows] * 0.5 + half_i)
            a = jnp.exp2(tr * coef + coef)
            v = jnp.maximum(1.0 - a * a, 1e-37)
            drive = (v * lax.rsqrt(v)) * ((ti * 0.5 + 0.5) * xp_ref[rows])
            if j == 0:
                h, prod = drive, a
            else:
                h, prod = a * h + drive, prod * a
            loc[b, rows] = h
            cum[b, rows] = prod
        start = jnp.zeros((1, HD), F32)
        gain = jnp.ones((1, HD), F32)
        starts, gains = [], []
        for s in range(8):
            starts.append(start)
            gains.append(gain)
            start = prod[s : s + 1] * start + h[s : s + 1]
            gain = gain * prod[s : s + 1]
        segc[b] = jnp.concatenate(starts, axis=0)
        segp[b] = jnp.concatenate(gains, axis=0)
        rowtot[c, y, 0, b - c * PER] = gain
        rowtot[c, y, 1, b - c * PER] = start

    def row_copy(c, k):
        return pltpu.make_async_remote_copy(
            src_ref=rowtot.at[c, y], dst_ref=rowtot.at[c, y],
            send_sem=row_send.at[c, k - 1], recv_sem=row_recv.at[c, y],
            device_id={"seq": z * COLS + (y + k) % COLS}, device_id_type=MESH,
        )

    def row_arrival(c, src):
        return pltpu.make_async_remote_copy(
            src_ref=rowtot.at[c, src], dst_ref=rowtot.at[c, src],
            send_sem=row_send.at[c, 0], recv_sem=row_recv.at[c, src],
            device_id={"seq": me}, device_id_type=MESH,
        )

    def col_copy(c, to):
        return pltpu.make_async_remote_copy(
            src_ref=coltot.at[c, z], dst_ref=coltot.at[c, z],
            send_sem=col_send.at[c, to], recv_sem=col_recv.at[c, z],
            device_id={"seq": to * COLS + y}, device_id_type=MESH,
        )

    def col_arrival(c, src):
        return pltpu.make_async_remote_copy(
            src_ref=coltot.at[c, src], dst_ref=coltot.at[c, src],
            send_sem=col_send.at[c, 0], recv_sem=col_recv.at[c, src],
            device_id={"seq": me}, device_id_type=MESH,
        )

    def send_row(c):
        for k in range(1, COLS):
            row_copy(c, k).start()

    def row_totals(c):
        for k in range(1, COLS):
            row_arrival(c, (y + k) % COLS).wait_recv()
        prod, state = rowtot[c, 0, 0], rowtot[c, 0, 1]
        before_p, before_s = jnp.ones_like(prod), jnp.zeros_like(state)
        for s in range(1, COLS):
            here = s <= y
            before_p = jnp.where(here, prod, before_p)
            before_s = jnp.where(here, state, before_s)
            prod, state = prod * rowtot[c, s, 0], rowtot[c, s, 0] * state + rowtot[c, s, 1]
        rowpre[c, 0] = before_p
        rowpre[c, 1] = before_s
        coltot[c, z, 0] = prod
        coltot[c, z, 1] = state
        for to in range(1, ROWS):
            @pl.when(to > z)
            def _():
                col_copy(c, to).start()

    def hidden(c):
        carry[...] = jnp.zeros(carry.shape, F32)
        for src in range(ROWS - 1):
            @pl.when(src < z)
            def _():
                col_arrival(c, src).wait_recv()
                carry[...] = coltot[c, src, 0] * carry[...] + coltot[c, src, 1]
        carry[...] = rowpre[c, 0] * carry[...] + rowpre[c, 1]
        total = None
        for i in range(PER):
            b = c * PER + i
            g = segc[b] + segp[b] * carry[i]
            value = loc[b].reshape(32, 8, HD) + cum[b].reshape(32, 8, HD) * g[None]
            value = value.reshape(TOK, HD).astype(BF16)
            hid[b] = value
            part = jnp.dot(value, wkv[b], preferred_element_type=F32)
            total = part if total is None else total + part
        if c == 0:
            kvacc[...] = total
        else:
            kvacc[...] += total

    for load in loads[0]:
        load.wait()
    gates(0, xp_a, lr_a, li_a)
    for c in range(CHUNKS):
        if c + 1 < CHUNKS:
            for load in loads[c + 1]:
                load.wait()

        def pair(i, _, c=c):
            b = c * PER + 2 * i
            gates(b + 1, xp_b, lr_b, li_b)
            scan(b, c, xp_a, lr_a, li_a)
            gates(jnp.minimum(b + 2, HEADS - 1), xp_a, lr_a, li_a)
            scan(b + 1, c, xp_b, lr_b, li_b)
            return 0

        lax.fori_loop(0, PER // 2, pair, 0)
        if c == 0:
            pl.semaphore_wait(barrier, COLS + ROWS - 2)
        send_row(c)
        if c >= 2:
            row_totals(c - 2)
    load_kv.wait()
    row_totals(CHUNKS - 2)
    row_totals(CHUNKS - 1)
    for c in range(CHUNKS):
        hidden(c)
    kv[0, :HD] = kvacc[:, :HD].astype(BF16)
    kv[0, HD:] = kvacc[:, HD:].astype(BF16)

    halo = Halo(kv, halo_send, halo_recv, z, y)
    halo.each(halo.own)

    def attend(offsets, group):
        place, n = PLACE[offsets[0]], len(offsets)
        nk, count, height = n * HD, HEADS // group, group * TOK
        first = offsets[0] == 0
        bias = bias0 if first else bias8 if offsets[0] == 8 else None

        def rows(g):
            return pl.ds(pl.multiple_of(g * height, height), height)

        def qk(g, s):
            queries = hid[pl.ds(g * group, group)].reshape(height, HD)
            keys = kv[place : place + n, :HD].reshape(nk, HD)
            value = lax.dot_general(
                queries, keys, (((1,), (1,)), ((), ())), preferred_element_type=F32
            )
            if bias is not None:
                masked = value[:, :HD].reshape(group, TOK, HD) + bias[...][None]
                masked = masked.reshape(height, HD)
                value = masked if n == 1 else jnp.concatenate([masked, value[:, HD:]], axis=1)
            s[:height, :nk] = value

        def soft(g, s, p, al):
            value = s[:height, :nk]
            r = rows(g)
            top = jnp.broadcast_to(jnp.max(value, axis=1, keepdims=True), (height, 128))
            if not first:
                before = m[r]
                top = jnp.maximum(before, top)
                alpha = jnp.exp2((before - top) * SCALE2)
                al[:height] = alpha
            m[r] = top
            shift = top * SCALE2
            part = None
            for j in range(nk // 128):
                e = jnp.exp2(value[:, 128 * j : 128 * j + 128] * SCALE2 - shift)
                p[:height, 128 * j : 128 * j + 128] = e.astype(BF16)
                part = e if part is None else part + e
            l[r] = part if first else l[r] * alpha + part

        def pv(g, p, al):
            r = rows(g)
            values = kv[place : place + n, HD:].reshape(nk, HD)
            new = jnp.dot(p[:height, :nk], values, preferred_element_type=F32)
            if first:
                acc[r] = new
            else:
                alpha = al[:height]
                acc[r] = acc[r] * jnp.concatenate([alpha, alpha], axis=1) + new

        qk(0, s_a)
        qk(1, s_b)
        soft(0, s_a, p_a, al_a)

        def body(i, _):
            g = 2 * i + 1
            qk(g + 1, s_a)
            pv(g - 1, p_a, al_a)
            soft(g, s_b, p_b, al_b)
            qk(g + 2, s_b)
            pv(g, p_b, al_b)
            soft(g + 1, s_a, p_a, al_a)
            return 0

        lax.fori_loop(0, count // 2 - 1, body, 0)
        pv(count - 2, p_a, al_a)
        soft(count - 1, s_b, p_b, al_b)
        pv(count - 1, p_b, al_b)

    attend((0,), 4)
    for c in range(CHUNKS):
        for k in range(1, COLS):
            row_copy(c, k).wait_send()
        for to in range(1, ROWS):
            @pl.when(to > z)
            def _():
                col_copy(c, to).wait_send()

    halo.each(halo.first_row)
    for index, step in enumerate(STEPS):
        halo.need(step)

        @pl.when(me >= max(step))
        def _():
            attend(step, 4)

        if len(step) == 2:
            @pl.when((me >= min(step)) & (me < max(step)))
            def _():
                attend((min(step),), 1)

        if index == 0:
            halo.each(halo.second_row)
        if index == 1:
            halo.each(halo.last_row)

    perm[...] = permutation(True)

    def finish(i, _):
        for u in range(PER):
            h = PER * i + u
            r = pl.ds(pl.multiple_of(h * TOK, TOK), TOK)
            total = jnp.sum(l[r], axis=1, keepdims=True)
            o = (acc[r] * (1.0 / total)).astype(BF16)
            out[:, lanes(h)] = jnp.dot(perm[...], o, preferred_element_type=F32).astype(BF16)
        return 0

    lax.fori_loop(0, CHUNKS, finish, 0)
    halo.drain()


def on_device(inputs, recur_weight, input_weight, recur_bias, input_bias, decay_rate, kv_weight):
    hbm = pl.BlockSpec(memory_space=pltpu.HBM)
    vmem = pl.BlockSpec(memory_space=pltpu.VMEM)
    tile = pltpu.VMEM((TOK, HD), F32)
    dma = pltpu.SemaphoreType.DMA
    return pl.pallas_call(
        kernel,
        in_specs=[hbm] * 7,
        out_specs=vmem,
        out_shape=jax.ShapeDtypeStruct((TOK, D), BF16),
        scratch_shapes=[
            pltpu.VMEM((TOK, D), BF16),
            pltpu.VMEM((HEADS, HD, HD), BF16),
            pltpu.VMEM((HEADS, HD, HD), BF16),
            pltpu.VMEM((1, D), F32),
            pltpu.VMEM((1, D), F32),
            pltpu.VMEM((1, D), F32),
            pltpu.VMEM((HEADS, HD, 2 * HD), BF16),
            pltpu.VMEM((TOK, TOK), BF16),
            tile, tile, tile, tile, tile, tile,
            pltpu.VMEM((HEADS, TOK, HD), F32),
            pltpu.VMEM((HEADS, TOK, HD), F32),
            pltpu.VMEM((HEADS, 8, HD), F32),
            pltpu.VMEM((HEADS, 8, HD), F32),
            pltpu.VMEM((CHUNKS, COLS, 2, PER, 1, HD), F32),
            pltpu.VMEM((CHUNKS, 2, PER, 1, HD), F32),
            pltpu.VMEM((CHUNKS, ROWS, 2, PER, 1, HD), F32),
            pltpu.VMEM((PER, 1, HD), F32),
            pltpu.VMEM((HEADS, TOK, HD), BF16),
            pltpu.VMEM((TOK, 2 * HD), F32),
            pltpu.VMEM((9, 2 * HD, HD), BF16),
            tile, tile,
            pltpu.VMEM((HEADS * TOK, 128), F32),
            pltpu.VMEM((HEADS * TOK, 128), F32),
            pltpu.VMEM((HEADS * TOK, HD), F32),
            pltpu.VMEM((4 * TOK, 2 * HD), F32),
            pltpu.VMEM((4 * TOK, 2 * HD), F32),
            pltpu.VMEM((4 * TOK, 2 * HD), BF16),
            pltpu.VMEM((4 * TOK, 2 * HD), BF16),
            pltpu.VMEM((4 * TOK, 128), F32),
            pltpu.VMEM((4 * TOK, 128), F32),
            dma((3 * CHUNKS + 4,)),
            dma((CHUNKS, COLS - 1)),
            dma((CHUNKS, COLS)),
            dma((CHUNKS, ROWS)),
            dma((CHUNKS, ROWS)),
            dma((24,)),
            dma((9, 2)),
        ],
        compiler_params=pltpu.CompilerParams(
            collective_id=0, has_side_effects=True, vmem_limit_bytes=51 * 1024 * 1024
        ),
        name="layer",
    )(
        inputs, recur_weight, input_weight, recur_bias[None], input_bias[None],
        decay_rate[None], kv_weight.reshape(HEADS, HD, 2 * HD),
    )


def solution(mesh):
    placed = (P(("batch", "seq"), None), P(), P(), P(), P(), P(), P())
    return jax.shard_map(
        on_device, mesh=mesh, in_specs=placed, out_specs=P(("batch", "seq"), None), check_vma=False
    )
```

```python
import math

import jax
import jax.numpy as jnp
from jax import lax
from jax.experimental import pallas as pl
from jax.experimental.pallas import tpu as pltpu
from jax.sharding import PartitionSpec as P

TOK = 256
D = 4096
HD = 256
HEADS = 16
ROWS = 8
COLS = 4
CHUNKS = 4
PER = HEADS // CHUNKS
PARTS = 4
KEYS = range(PARTS // 2)
VALUES = range(PARTS // 2, PARTS)
LOG2E = math.log2(math.e)
SCALE2 = (HD ** -0.5) * LOG2E
NEG = -1e30
F32 = jnp.float32
BF16 = jnp.bfloat16
MESH = pl.DeviceIdType.MESH

STEPS = ((4,), (1, 3), (8, 5), (2, 7), (6,))
PLACE = {0: 0}
for _step in STEPS:
    for _o in _step:
        PLACE[_o] = len(PLACE)


def token_of(row):
    return (row % 8) * 32 + row // 8


def permutation(transposed):
    rows = lax.broadcasted_iota(jnp.int32, (TOK, TOK), 1 if transposed else 0)
    toks = lax.broadcasted_iota(jnp.int32, (TOK, TOK), 0 if transposed else 1)
    return (token_of(rows) == toks).astype(F32).astype(BF16)


def row_distance(o, y):
    return (o - y + COLS - 1) // COLS


class Halo:
    def __init__(self, kv, send, recv, z, y):
        self.kv, self.send, self.recv, self.z, self.y = kv, send, recv, z, y
        self.count = [0] * COLS
        self.waited = [set() for _ in range(COLS)]
        self.started = [[] for _ in range(COLS)]

    def half(self, o, part):
        size = 2 * HD // PARTS
        return self.kv.at[PLACE[o], pl.ds(part * size, size)]

    def copy(self, index, src, dst, part, dz, dst_y):
        return pltpu.make_async_remote_copy(
            src_ref=self.half(src, part),
            dst_ref=self.half(dst, part),
            send_sem=self.send.at[index],
            recv_sem=self.recv.at[PLACE[dst], part],
            device_id={"seq": (self.z + dz) * COLS + dst_y},
            device_id_type=MESH,
        )

    def start(self, yy, src, part, dz, dst_y):
        dst = src + dz * COLS + dst_y - yy
        low = row_distance(src, yy)
        high = ROWS - 2 if dz else ROWS - 1
        index = self.count[yy]
        self.count[yy] += 1
        args = (index, src, dst, part, dz, dst_y)

        @pl.when((self.z >= low) & (self.z <= high))
        def _():
            self.copy(*args).start()

        self.started[yy].append((low, high, args))

    def arrive(self, yy, o, part):
        if (o, part) in self.waited[yy]:
            return
        self.waited[yy].add((o, part))

        @pl.when(self.z >= row_distance(o, yy))
        def _():
            pltpu.make_async_remote_copy(
                src_ref=self.half(o, part),
                dst_ref=self.half(o, part),
                send_sem=self.send.at[0],
                recv_sem=self.recv.at[PLACE[o], part],
                device_id={"seq": self.z * COLS + self.y},
                device_id_type=MESH,
            ).wait_recv()

    def each(self, fn):
        for yy in range(COLS):
            @pl.when(self.y == yy)
            def _():
                fn(yy)

    def own(self, yy):
        for part in range(PARTS):
            self.start(yy, 0, part, 1, yy)
            if yy < COLS - 1:
                self.start(yy, 0, part, 0, yy + 1)
            if yy == 0:
                self.start(yy, 0, part, 0, COLS - 1)

    def first_row(self, yy):
        for part in range(PARTS):
            self.arrive(yy, 4, part)
            self.start(yy, 4, part, 1, yy)
            self.start(yy, 4, part, 0, (yy + 1) % COLS)
            self.start(yy, 4, part, 0, (yy - 1) % COLS)
            if yy == 1 and part in KEYS:
                self.arrive(yy, 1, part)
                self.start(yy, 1, part, 0, 2)
            if yy == 2:
                self.arrive(yy, 1, part)
                self.start(yy, 1, part, 0, 3)
            if yy == 3 and part in VALUES:
                self.arrive(yy, 3, part)
                self.start(yy, 3, part, 0, 2)

    def second_row(self, yy):
        left, right = (yy - 1) % COLS, (yy + 1) % COLS
        from_left, from_right = 4 + yy - left, 4 + yy - right
        for part in range(PARTS):
            self.arrive(yy, 8, part)
            if yy >= 1:
                self.start(yy, 8, part, 0, yy - 1)
            if yy == COLS - 1:
                self.start(yy, 8, part, 0, 0)
            if part in KEYS:
                self.arrive(yy, from_left, part)
                self.start(yy, from_left, part, 0, right)
            else:
                self.arrive(yy, from_right, part)
                self.start(yy, from_right, part, 0, left)

    def last_row(self, yy):
        if yy == 0:
            for part in VALUES:
                self.arrive(yy, 5, part)
                self.start(yy, 5, part, 0, 1)
        if yy == 1:
            for part in range(PARTS):
                self.arrive(yy, 7, part)
                self.start(yy, 7, part, 0, 0)
        if yy == 2:
            for part in KEYS:
                self.arrive(yy, 7, part)
                self.start(yy, 7, part, 0, 1)

    def need(self, step):
        def fn(yy):
            for o in step:
                for part in range(PARTS):
                    self.arrive(yy, o, part)

        self.each(fn)

    def drain(self):
        def fn(yy):
            for low, high, args in self.started[yy]:
                @pl.when((self.z >= low) & (self.z <= high))
                def _(args=args):
                    self.copy(*args).wait_send()

        self.each(fn)


def kernel(
    x_hbm, wr_hbm, wi_hbm, br_hbm, bi_hbm, rate_hbm, wkv_hbm, out,
    x, wr, wi, br, bi, rate, wkv, perm, back, xp_a, lr_a, li_a, xp_b, lr_b, li_b, loc, cum, segc, segp,
    rowtot, rowpre, coltot, carry, hid, kvacc, kv, bias0, bias8,
    m, l, acc, s_a, s_b, p_a, p_b, al_a, al_b,
    load_sem, row_send, row_recv, col_send, col_recv, halo_send, halo_recv,
):
    me = lax.axis_index("seq")
    z, y = me // COLS, me % COLS

    loads = []
    for c in range(CHUNKS):
        cols, blocks = pl.ds(c * PER * HD, PER * HD), pl.ds(c * PER, PER)
        loads.append([
            pltpu.make_async_copy(x_hbm.at[:, cols], x.at[:, cols], load_sem.at[3 * c]),
            pltpu.make_async_copy(wr_hbm.at[blocks], wr.at[blocks], load_sem.at[3 * c + 1]),
            pltpu.make_async_copy(wi_hbm.at[blocks], wi.at[blocks], load_sem.at[3 * c + 2]),
        ])
    load_kv = pltpu.make_async_copy(wkv_hbm, wkv, load_sem.at[3 * CHUNKS])
    small = [
        pltpu.make_async_copy(src, dst, load_sem.at[3 * CHUNKS + 1 + k])
        for k, (src, dst) in enumerate([(br_hbm, br), (bi_hbm, bi), (rate_hbm, rate)])
    ]
    loads[0] += small
    for group in loads:
        for load in group:
            load.start()
    load_kv.start()

    barrier = pltpu.get_barrier_semaphore()
    for k in range(1, COLS):
        pl.semaphore_signal(
            barrier, inc=1, device_id={"seq": z * COLS + (y + k) % COLS}, device_id_type=MESH
        )
    for k in range(1, ROWS):
        pl.semaphore_signal(
            barrier, inc=1, device_id={"seq": ((z + k) % ROWS) * COLS + y}, device_id_type=MESH
        )

    perm[...] = permutation(False)
    back[...] = permutation(True)
    kt = token_of(lax.broadcasted_iota(jnp.int32, (TOK, TOK), 1))
    qt = token_of(lax.broadcasted_iota(jnp.int32, (TOK, TOK), 0))
    bias0[...] = jnp.where(kt <= qt, 0.0, NEG)
    bias8[...] = jnp.where(kt <= qt, NEG, 0.0)

    def lanes(b):
        return pl.ds(pl.multiple_of(b * HD, HD), HD)

    def gates(b, xp_ref, lr_ref, li_ref):
        xp = jnp.dot(perm[...], x[:, lanes(b)], preferred_element_type=F32)
        xb = xp.astype(BF16)
        xp_ref[...] = xp
        lr_ref[...] = jnp.dot(xb, wr[b], preferred_element_type=F32)
        li_ref[...] = jnp.dot(xb, wi[b], preferred_element_type=F32)

    def scan(b, c, xp_ref, lr_ref, li_ref):
        half_r, half_i = br[:, lanes(b)] * 0.5, bi[:, lanes(b)] * 0.5
        coef = rate[:, lanes(b)] * (-4.0 * LOG2E)
        for j in range(32):
            rows = slice(8 * j, 8 * j + 8)
            tr = jnp.tanh(lr_ref[rows] * 0.5 + half_r)
            ti = jnp.tanh(li_ref[rows] * 0.5 + half_i)
            a = jnp.exp2(tr * coef + coef)
            v = jnp.maximum(1.0 - a * a, 1e-37)
            drive = (v * lax.rsqrt(v)) * ((ti * 0.5 + 0.5) * xp_ref[rows])
            if j == 0:
                h, prod = drive, a
            else:
                h, prod = a * h + drive, prod * a
            loc[b, rows] = h
            cum[b, rows] = prod
        start = jnp.zeros((1, HD), F32)
        gain = jnp.ones((1, HD), F32)
        starts, gains = [], []
        for s in range(8):
            starts.append(start)
            gains.append(gain)
            start = prod[s : s + 1] * start + h[s : s + 1]
            gain = gain * prod[s : s + 1]
        segc[b] = jnp.concatenate(starts, axis=0)
        segp[b] = jnp.concatenate(gains, axis=0)
        rowtot[c, y, 0, b - c * PER] = gain
        rowtot[c, y, 1, b - c * PER] = start

    def row_copy(c, k):
        return pltpu.make_async_remote_copy(
            src_ref=rowtot.at[c, y], dst_ref=rowtot.at[c, y],
            send_sem=row_send.at[c, k - 1], recv_sem=row_recv.at[c, y],
            device_id={"seq": z * COLS + (y + k) % COLS}, device_id_type=MESH,
        )

    def row_arrival(c, src):
        return pltpu.make_async_remote_copy(
            src_ref=rowtot.at[c, src], dst_ref=rowtot.at[c, src],
            send_sem=row_send.at[c, 0], recv_sem=row_recv.at[c, src],
            device_id={"seq": me}, device_id_type=MESH,
        )

    def col_copy(c, to):
        return pltpu.make_async_remote_copy(
            src_ref=coltot.at[c, z], dst_ref=coltot.at[c, z],
            send_sem=col_send.at[c, to], recv_sem=col_recv.at[c, z],
            device_id={"seq": to * COLS + y}, device_id_type=MESH,
        )

    def col_arrival(c, src):
        return pltpu.make_async_remote_copy(
            src_ref=coltot.at[c, src], dst_ref=coltot.at[c, src],
            send_sem=col_send.at[c, 0], recv_sem=col_recv.at[c, src],
            device_id={"seq": me}, device_id_type=MESH,
        )

    def send_row(c):
        for k in range(1, COLS):
            row_copy(c, k).start()

    def row_totals(c):
        for k in range(1, COLS):
            row_arrival(c, (y + k) % COLS).wait_recv()
        prod, state = rowtot[c, 0, 0], rowtot[c, 0, 1]
        before_p, before_s = jnp.ones_like(prod), jnp.zeros_like(state)
        for s in range(1, COLS):
            here = s <= y
            before_p = jnp.where(here, prod, before_p)
            before_s = jnp.where(here, state, before_s)
            prod, state = prod * rowtot[c, s, 0], rowtot[c, s, 0] * state + rowtot[c, s, 1]
        rowpre[c, 0] = before_p
        rowpre[c, 1] = before_s
        coltot[c, z, 0] = prod
        coltot[c, z, 1] = state
        for to in range(1, ROWS):
            @pl.when(to > z)
            def _():
                col_copy(c, to).start()

    def hidden(c):
        carry[...] = jnp.zeros(carry.shape, F32)
        for src in range(ROWS - 1):
            @pl.when(src < z)
            def _():
                col_arrival(c, src).wait_recv()
                carry[...] = coltot[c, src, 0] * carry[...] + coltot[c, src, 1]
        carry[...] = rowpre[c, 0] * carry[...] + rowpre[c, 1]
        total = None
        for i in range(PER):
            b = c * PER + i
            g = segc[b] + segp[b] * carry[i]
            value = loc[b].reshape(32, 8, HD) + cum[b].reshape(32, 8, HD) * g[None]
            value = value.reshape(TOK, HD).astype(BF16)
            hid[b] = value
            part = jnp.dot(value, wkv[b], preferred_element_type=F32)
            total = part if total is None else total + part
        if c == 0:
            kvacc[...] = total
        else:
            kvacc[...] += total

    for load in loads[0]:
        load.wait()
    gates(0, xp_a, lr_a, li_a)
    for c in range(CHUNKS):
        if c + 1 < CHUNKS:
            for load in loads[c + 1]:
                load.wait()

        def pair(i, _, c=c):
            b = c * PER + 2 * i
            gates(b + 1, xp_b, lr_b, li_b)
            scan(b, c, xp_a, lr_a, li_a)
            gates(jnp.minimum(b + 2, HEADS - 1), xp_a, lr_a, li_a)
            scan(b + 1, c, xp_b, lr_b, li_b)
            return 0

        for i in range(PER // 2):
            pair(i, 0)
        if c == 0:
            pl.semaphore_wait(barrier, COLS + ROWS - 2)
        send_row(c)
        if c >= 2:
            row_totals(c - 2)
    load_kv.wait()
    row_totals(CHUNKS - 2)
    row_totals(CHUNKS - 1)
    for c in range(CHUNKS):
        hidden(c)
    kv[0, :HD] = kvacc[:, :HD].astype(BF16)
    kv[0, HD:] = kvacc[:, HD:].astype(BF16)

    halo = Halo(kv, halo_send, halo_recv, z, y)
    halo.each(halo.own)

    def finish(h, weighted, total):
        total = jnp.sum(total, axis=1, keepdims=True)
        o = (weighted * (1.0 / total)).astype(BF16)
        out[:, lanes(h)] = jnp.dot(back[...], o, preferred_element_type=F32).astype(BF16)

    def attend(offsets, group, final=False):
        place, n = PLACE[offsets[0]], len(offsets)
        nk, count, height = n * HD, HEADS // group, group * TOK
        first = offsets[0] == 0
        bias = bias0 if first else bias8 if offsets[0] == 8 else None

        def rows(g):
            return pl.ds(pl.multiple_of(g * height, height), height)

        def qk(g, s):
            queries = hid[pl.ds(g * group, group)].reshape(height, HD)
            keys = kv[place : place + n, :HD].reshape(nk, HD)
            value = lax.dot_general(
                queries, keys, (((1,), (1,)), ((), ())), preferred_element_type=F32
            )
            if bias is not None:
                masked = value[:, :HD].reshape(group, TOK, HD) + bias[...][None]
                masked = masked.reshape(height, HD)
                value = masked if n == 1 else jnp.concatenate([masked, value[:, HD:]], axis=1)
            s[:height, :nk] = value

        def soft(g, s, p, al):
            value = s[:height, :nk]
            r = rows(g)
            top = jnp.broadcast_to(jnp.max(value, axis=1, keepdims=True), (height, 128))
            if not first:
                before = m[r]
                top = jnp.maximum(before, top)
                alpha = jnp.exp2((before - top) * SCALE2)
                al[:height] = alpha
            m[r] = top
            shift = top * SCALE2
            part = None
            for j in range(nk // 128):
                e = jnp.exp2(value[:, 128 * j : 128 * j + 128] * SCALE2 - shift)
                p[:height, 128 * j : 128 * j + 128] = e.astype(BF16)
                part = e if part is None else part + e
            l[r] = part if first else l[r] * alpha + part

        def pv(g, p, al):
            r = rows(g)
            values = kv[place : place + n, HD:].reshape(nk, HD)
            new = jnp.dot(p[:height, :nk], values, preferred_element_type=F32)
            if first:
                acc[r] = new
            else:
                alpha = al[:height]
                new = acc[r] * jnp.concatenate([alpha, alpha], axis=1) + new
                if not final:
                    acc[r] = new
                    return
                total = l[r]
                for u in range(group):
                    part = slice(u * TOK, u * TOK + TOK)
                    finish(g * group + u, new[part], total[part])

        qk(0, s_a)
        qk(1, s_b)
        soft(0, s_a, p_a, al_a)

        def body(i, _):
            g = 2 * i + 1
            qk(g + 1, s_a)
            pv(g - 1, p_a, al_a)
            soft(g, s_b, p_b, al_b)
            qk(g + 2, s_b)
            pv(g, p_b, al_b)
            soft(g + 1, s_a, p_a, al_a)
            return 0

        lax.fori_loop(0, count // 2 - 1, body, 0)
        pv(count - 2, p_a, al_a)
        soft(count - 1, s_b, p_b, al_b)
        pv(count - 1, p_b, al_b)

    attend((0,), 4)
    for c in range(CHUNKS):
        for k in range(1, COLS):
            row_copy(c, k).wait_send()
        for to in range(1, ROWS):
            @pl.when(to > z)
            def _():
                col_copy(c, to).wait_send()

    halo.each(halo.first_row)
    for index, step in enumerate(STEPS):
        halo.need(step)

        @pl.when(me >= max(step))
        def _():
            attend(step, 4, final=index == len(STEPS) - 1)

        if len(step) == 2:
            @pl.when((me >= min(step)) & (me < max(step)))
            def _():
                attend((min(step),), 1)

        if index == 0:
            halo.each(halo.second_row)
        if index == 1:
            halo.each(halo.last_row)

    def finish_four(i, _):
        for u in range(PER):
            h = PER * i + u
            r = pl.ds(pl.multiple_of(h * TOK, TOK), TOK)
            finish(h, acc[r], l[r])
        return 0

    @pl.when(me < STEPS[-1][0])
    def _():
        lax.fori_loop(0, CHUNKS, finish_four, 0)

    halo.drain()


def keep(v):
    return pltpu.with_memory_space_constraint(v, pltpu.HBM)


def on_device(inputs, recur_weight, input_weight, recur_bias, input_bias, decay_rate, kv_weight):
    hbm = pl.BlockSpec(memory_space=pltpu.HBM)
    vmem = pl.BlockSpec(memory_space=pltpu.VMEM)
    tile = pltpu.VMEM((TOK, HD), F32)
    dma = pltpu.SemaphoreType.DMA
    return pl.pallas_call(
        kernel,
        in_specs=[hbm] * 7,
        out_specs=vmem,
        out_shape=jax.ShapeDtypeStruct((TOK, D), BF16),
        scratch_shapes=[
            pltpu.VMEM((TOK, D), BF16),
            pltpu.VMEM((HEADS, HD, HD), BF16),
            pltpu.VMEM((HEADS, HD, HD), BF16),
            pltpu.VMEM((1, D), F32),
            pltpu.VMEM((1, D), F32),
            pltpu.VMEM((1, D), F32),
            pltpu.VMEM((HEADS, HD, 2 * HD), BF16),
            pltpu.VMEM((TOK, TOK), BF16),
            pltpu.VMEM((TOK, TOK), BF16),
            tile, tile, tile, tile, tile, tile,
            pltpu.VMEM((HEADS, TOK, HD), F32),
            pltpu.VMEM((HEADS, TOK, HD), F32),
            pltpu.VMEM((HEADS, 8, HD), F32),
            pltpu.VMEM((HEADS, 8, HD), F32),
            pltpu.VMEM((CHUNKS, COLS, 2, PER, 1, HD), F32),
            pltpu.VMEM((CHUNKS, 2, PER, 1, HD), F32),
            pltpu.VMEM((CHUNKS, ROWS, 2, PER, 1, HD), F32),
            pltpu.VMEM((PER, 1, HD), F32),
            pltpu.VMEM((HEADS, TOK, HD), BF16),
            pltpu.VMEM((TOK, 2 * HD), F32),
            pltpu.VMEM((9, 2 * HD, HD), BF16),
            tile, tile,
            pltpu.VMEM((HEADS * TOK, 128), F32),
            pltpu.VMEM((HEADS * TOK, 128), F32),
            pltpu.VMEM((HEADS * TOK, HD), F32),
            pltpu.VMEM((4 * TOK, 2 * HD), F32),
            pltpu.VMEM((4 * TOK, 2 * HD), F32),
            pltpu.VMEM((4 * TOK, 2 * HD), BF16),
            pltpu.VMEM((4 * TOK, 2 * HD), BF16),
            pltpu.VMEM((4 * TOK, 128), F32),
            pltpu.VMEM((4 * TOK, 128), F32),
            dma((3 * CHUNKS + 4,)),
            dma((CHUNKS, COLS - 1)),
            dma((CHUNKS, COLS)),
            dma((CHUNKS, ROWS)),
            dma((CHUNKS, ROWS)),
            dma((17 * PARTS // 2,)),
            dma((9, PARTS)),
        ],
        compiler_params=pltpu.CompilerParams(
            collective_id=0, has_side_effects=True, vmem_limit_bytes=51 * 1024 * 1024
        ),
        name="layer",
    )(
        inputs, recur_weight, input_weight, keep(recur_bias[None]), keep(input_bias[None]),
        keep(decay_rate[None]), kv_weight.reshape(HEADS, HD, 2 * HD),
    )


def solution(mesh):
    placed = (P(("batch", "seq"), None), P(), P(), P(), P(), P(), P())
    return jax.shard_map(
        on_device, mesh=mesh, in_specs=placed, out_specs=P(("batch", "seq"), None), check_vma=False
    )
```

```python
import math

import jax
import jax.numpy as jnp
from jax import lax
from jax.experimental import pallas as pl
from jax.experimental.pallas import tpu as pltpu
from jax.sharding import PartitionSpec as P

TOK = 256
D = 4096
HD = 256
HEADS = 16
ROWS = 8
COLS = 4
CHUNKS = 4
PER = HEADS // CHUNKS
PARTS = 4
KEYS = range(PARTS // 2)
VALUES = range(PARTS // 2, PARTS)
LOG2E = math.log2(math.e)
SCALE2 = (HD ** -0.5) * LOG2E
NEG = -1e30
F32 = jnp.float32
BF16 = jnp.bfloat16
MESH = pl.DeviceIdType.MESH

STEPS = ((4,), (1, 3), (8, 5), (2, 7), (6,))
PLACE = {0: 0}
for _step in STEPS:
    for _o in _step:
        PLACE[_o] = len(PLACE)


def token_of(row):
    return (row % 8) * 32 + row // 8


def permutation(transposed):
    rows = lax.broadcasted_iota(jnp.int32, (TOK, TOK), 1 if transposed else 0)
    toks = lax.broadcasted_iota(jnp.int32, (TOK, TOK), 0 if transposed else 1)
    return (token_of(rows) == toks).astype(F32).astype(BF16)


def row_distance(o, y):
    return (o - y + COLS - 1) // COLS


class Halo:
    def __init__(self, kv, send, recv, z, y):
        self.kv, self.send, self.recv, self.z, self.y = kv, send, recv, z, y
        self.count = [0] * COLS
        self.waited = [set() for _ in range(COLS)]
        self.started = [[] for _ in range(COLS)]

    def half(self, o, part):
        size = 2 * HD // PARTS
        return self.kv.at[PLACE[o], pl.ds(part * size, size)]

    def copy(self, index, src, dst, part, dz, dst_y):
        return pltpu.make_async_remote_copy(
            src_ref=self.half(src, part),
            dst_ref=self.half(dst, part),
            send_sem=self.send.at[index],
            recv_sem=self.recv.at[PLACE[dst], part],
            device_id={"seq": (self.z + dz) * COLS + dst_y},
            device_id_type=MESH,
        )

    def start(self, yy, src, part, dz, dst_y):
        dst = src + dz * COLS + dst_y - yy
        low = row_distance(src, yy)
        high = ROWS - 2 if dz else ROWS - 1
        index = self.count[yy]
        self.count[yy] += 1
        args = (index, src, dst, part, dz, dst_y)

        @pl.when((self.z >= low) & (self.z <= high))
        def _():
            self.copy(*args).start()

        self.started[yy].append((low, high, args))

    def arrive(self, yy, o, part):
        if (o, part) in self.waited[yy]:
            return
        self.waited[yy].add((o, part))

        @pl.when(self.z >= row_distance(o, yy))
        def _():
            pltpu.make_async_remote_copy(
                src_ref=self.half(o, part),
                dst_ref=self.half(o, part),
                send_sem=self.send.at[0],
                recv_sem=self.recv.at[PLACE[o], part],
                device_id={"seq": self.z * COLS + self.y},
                device_id_type=MESH,
            ).wait_recv()

    def each(self, fn):
        for yy in range(COLS):
            @pl.when(self.y == yy)
            def _():
                fn(yy)

    def own(self, yy):
        for part in range(PARTS):
            self.start(yy, 0, part, 1, yy)
            if yy < COLS - 1:
                self.start(yy, 0, part, 0, yy + 1)
            if yy == 0:
                self.start(yy, 0, part, 0, COLS - 1)

    def first_row(self, yy):
        for part in range(PARTS):
            self.arrive(yy, 4, part)
            self.start(yy, 4, part, 1, yy)
            self.start(yy, 4, part, 0, (yy + 1) % COLS)
            self.start(yy, 4, part, 0, (yy - 1) % COLS)

    def second_row(self, yy):
        left, right = (yy - 1) % COLS, (yy + 1) % COLS
        from_left, from_right = 4 + yy - left, 4 + yy - right
        for part in range(PARTS):
            if yy == 1 and part in KEYS:
                self.arrive(yy, 1, part)
                self.start(yy, 1, part, 0, 2)
            if yy == 2:
                self.arrive(yy, 1, part)
                self.start(yy, 1, part, 0, 3)
            if yy == 3 and part in VALUES:
                self.arrive(yy, 3, part)
                self.start(yy, 3, part, 0, 2)
        for part in range(PARTS):
            self.arrive(yy, 8, part)
            if yy >= 1:
                self.start(yy, 8, part, 0, yy - 1)
            if yy == COLS - 1:
                self.start(yy, 8, part, 0, 0)
            if part in KEYS:
                self.arrive(yy, from_left, part)
                self.start(yy, from_left, part, 0, right)
            else:
                self.arrive(yy, from_right, part)
                self.start(yy, from_right, part, 0, left)

    def last_row(self, yy):
        if yy == 0:
            for part in VALUES:
                self.arrive(yy, 5, part)
                self.start(yy, 5, part, 0, 1)
        if yy == 1:
            for part in range(PARTS):
                self.arrive(yy, 7, part)
                self.start(yy, 7, part, 0, 0)
        if yy == 2:
            for part in KEYS:
                self.arrive(yy, 7, part)
                self.start(yy, 7, part, 0, 1)

    def need(self, step):
        def fn(yy):
            for o in step:
                for part in range(PARTS):
                    self.arrive(yy, o, part)

        self.each(fn)

    def drain(self):
        def fn(yy):
            for low, high, args in self.started[yy]:
                @pl.when((self.z >= low) & (self.z <= high))
                def _(args=args):
                    self.copy(*args).wait_send()

        self.each(fn)


def kernel(
    x_hbm, wr_hbm, wi_hbm, br_hbm, bi_hbm, rate_hbm, wkv_hbm, out,
    x, wr, wi, br, bi, rate, wkv, perm, back, xp_a, lr_a, li_a, xp_b, lr_b, li_b, loc, cum, segc, segp,
    rowtot, rowpre, coltot, carry, hid, kvacc, kv, bias0, bias8,
    m, l, acc, s_a, s_b, p_a, p_b, al_a, al_b,
    load_sem, row_send, row_recv, col_send, col_recv, halo_send, halo_recv,
):
    me = lax.axis_index("seq")
    z, y = me // COLS, me % COLS

    loads = []
    for c in range(CHUNKS):
        cols, blocks = pl.ds(c * PER * HD, PER * HD), pl.ds(c * PER, PER)
        loads.append([
            pltpu.make_async_copy(x_hbm.at[:, cols], x.at[:, cols], load_sem.at[3 * c]),
            pltpu.make_async_copy(wr_hbm.at[blocks], wr.at[blocks], load_sem.at[3 * c + 1]),
            pltpu.make_async_copy(wi_hbm.at[blocks], wi.at[blocks], load_sem.at[3 * c + 2]),
        ])
    load_kv = pltpu.make_async_copy(wkv_hbm, wkv, load_sem.at[3 * CHUNKS])
    small = [
        pltpu.make_async_copy(src, dst, load_sem.at[3 * CHUNKS + 1 + k])
        for k, (src, dst) in enumerate([(br_hbm, br), (bi_hbm, bi), (rate_hbm, rate)])
    ]
    loads[0] += small
    for group in loads:
        for load in group:
            load.start()
    load_kv.start()

    barrier = pltpu.get_barrier_semaphore()
    for k in range(1, COLS):
        pl.semaphore_signal(
            barrier, inc=1, device_id={"seq": z * COLS + (y + k) % COLS}, device_id_type=MESH
        )
    for k in range(1, ROWS):
        pl.semaphore_signal(
            barrier, inc=1, device_id={"seq": ((z + k) % ROWS) * COLS + y}, device_id_type=MESH
        )

    perm[...] = permutation(False)
    back[...] = permutation(True)
    kt = token_of(lax.broadcasted_iota(jnp.int32, (TOK, TOK), 1))
    qt = token_of(lax.broadcasted_iota(jnp.int32, (TOK, TOK), 0))
    bias0[...] = jnp.where(kt <= qt, 0.0, NEG)
    bias8[...] = jnp.where(kt <= qt, NEG, 0.0)

    def lanes(b):
        return pl.ds(pl.multiple_of(b * HD, HD), HD)

    def gates(b, xp_ref, lr_ref, li_ref):
        xp = jnp.dot(perm[...], x[:, lanes(b)], preferred_element_type=F32)
        xb = xp.astype(BF16)
        xp_ref[...] = xp
        lr_ref[...] = jnp.dot(xb, wr[b], preferred_element_type=F32)
        li_ref[...] = jnp.dot(xb, wi[b], preferred_element_type=F32)

    def scan(b, c, xp_ref, lr_ref, li_ref):
        half_r, half_i = br[:, lanes(b)] * 0.5, bi[:, lanes(b)] * 0.5
        coef = rate[:, lanes(b)] * (-4.0 * LOG2E)
        for j in range(32):
            rows = slice(8 * j, 8 * j + 8)
            tr = jnp.tanh(lr_ref[rows] * 0.5 + half_r)
            ti = jnp.tanh(li_ref[rows] * 0.5 + half_i)
            a = jnp.exp2(tr * coef + coef)
            v = jnp.maximum(1.0 - a * a, 1e-37)
            drive = (v * lax.rsqrt(v)) * ((ti * 0.5 + 0.5) * xp_ref[rows])
            if j == 0:
                h, prod = drive, a
            else:
                h, prod = a * h + drive, prod * a
            loc[b, rows] = h
            cum[b, rows] = prod
        start = jnp.zeros((1, HD), F32)
        gain = jnp.ones((1, HD), F32)
        starts, gains = [], []
        for s in range(8):
            starts.append(start)
            gains.append(gain)
            start = prod[s : s + 1] * start + h[s : s + 1]
            gain = gain * prod[s : s + 1]
        segc[b] = jnp.concatenate(starts, axis=0)
        segp[b] = jnp.concatenate(gains, axis=0)
        rowtot[c, y, 0, b - c * PER] = gain
        rowtot[c, y, 1, b - c * PER] = start

    def row_copy(c, k):
        return pltpu.make_async_remote_copy(
            src_ref=rowtot.at[c, y], dst_ref=rowtot.at[c, y],
            send_sem=row_send.at[c, k - 1], recv_sem=row_recv.at[c, y],
            device_id={"seq": z * COLS + (y + k) % COLS}, device_id_type=MESH,
        )

    def row_arrival(c, src):
        return pltpu.make_async_remote_copy(
            src_ref=rowtot.at[c, src], dst_ref=rowtot.at[c, src],
            send_sem=row_send.at[c, 0], recv_sem=row_recv.at[c, src],
            device_id={"seq": me}, device_id_type=MESH,
        )

    def col_copy(c, to):
        return pltpu.make_async_remote_copy(
            src_ref=coltot.at[c, z], dst_ref=coltot.at[c, z],
            send_sem=col_send.at[c, to], recv_sem=col_recv.at[c, z],
            device_id={"seq": to * COLS + y}, device_id_type=MESH,
        )

    def col_arrival(c, src):
        return pltpu.make_async_remote_copy(
            src_ref=coltot.at[c, src], dst_ref=coltot.at[c, src],
            send_sem=col_send.at[c, 0], recv_sem=col_recv.at[c, src],
            device_id={"seq": me}, device_id_type=MESH,
        )

    def send_row(c):
        for k in range(1, COLS):
            row_copy(c, k).start()

    def row_totals(c):
        for k in range(1, COLS):
            row_arrival(c, (y + k) % COLS).wait_recv()
        prod, state = rowtot[c, 0, 0], rowtot[c, 0, 1]
        before_p, before_s = jnp.ones_like(prod), jnp.zeros_like(state)
        for s in range(1, COLS):
            here = s <= y
            before_p = jnp.where(here, prod, before_p)
            before_s = jnp.where(here, state, before_s)
            prod, state = prod * rowtot[c, s, 0], rowtot[c, s, 0] * state + rowtot[c, s, 1]
        rowpre[c, 0] = before_p
        rowpre[c, 1] = before_s
        coltot[c, z, 0] = prod
        coltot[c, z, 1] = state
        for to in range(1, ROWS):
            @pl.when(to > z)
            def _():
                col_copy(c, to).start()

    def hidden(c):
        carry[...] = jnp.zeros(carry.shape, F32)
        for src in range(ROWS - 1):
            @pl.when(src < z)
            def _():
                col_arrival(c, src).wait_recv()
                carry[...] = coltot[c, src, 0] * carry[...] + coltot[c, src, 1]
        carry[...] = rowpre[c, 0] * carry[...] + rowpre[c, 1]
        total = None
        for i in range(PER):
            b = c * PER + i
            g = segc[b] + segp[b] * carry[i]
            value = loc[b].reshape(32, 8, HD) + cum[b].reshape(32, 8, HD) * g[None]
            value = value.reshape(TOK, HD).astype(BF16)
            hid[b] = value
            part = jnp.dot(value, wkv[b], preferred_element_type=F32)
            total = part if total is None else total + part
        if c == 0:
            kvacc[...] = total
        else:
            kvacc[...] += total

    for load in loads[0]:
        load.wait()
    gates(0, xp_a, lr_a, li_a)
    for c in range(CHUNKS):
        if c + 1 < CHUNKS:
            for load in loads[c + 1]:
                load.wait()

        def pair(i, _, c=c):
            b = c * PER + 2 * i
            gates(b + 1, xp_b, lr_b, li_b)
            scan(b, c, xp_a, lr_a, li_a)
            gates(jnp.minimum(b + 2, HEADS - 1), xp_a, lr_a, li_a)
            scan(b + 1, c, xp_b, lr_b, li_b)
            return 0

        for i in range(PER // 2):
            pair(i, 0)
        if c == 0:
            pl.semaphore_wait(barrier, COLS + ROWS - 2)
        send_row(c)
        if c >= 2:
            row_totals(c - 2)
    load_kv.wait()
    row_totals(CHUNKS - 2)
    row_totals(CHUNKS - 1)
    for c in range(CHUNKS):
        hidden(c)
    kv[0, :HD] = kvacc[:, :HD].astype(BF16)
    kv[0, HD:] = kvacc[:, HD:].astype(BF16)

    halo = Halo(kv, halo_send, halo_recv, z, y)
    halo.each(halo.own)

    def finish(h, weighted, total):
        total = jnp.sum(total, axis=1, keepdims=True)
        o = (weighted * (1.0 / total)).astype(BF16)
        out[:, lanes(h)] = jnp.dot(back[...], o, preferred_element_type=F32).astype(BF16)

    def attend(offsets, group, final=False):
        place, n = PLACE[offsets[0]], len(offsets)
        nk, count, height = n * HD, HEADS // group, group * TOK
        first = offsets[0] == 0
        bias = bias0 if first else bias8 if offsets[0] == 8 else None

        def rows(g):
            return pl.ds(pl.multiple_of(g * height, height), height)

        def qk(g, s):
            queries = hid[pl.ds(g * group, group)].reshape(height, HD)
            keys = kv[place : place + n, :HD].reshape(nk, HD)
            value = lax.dot_general(
                queries, keys, (((1,), (1,)), ((), ())), preferred_element_type=F32
            )
            if bias is not None:
                masked = value[:, :HD].reshape(group, TOK, HD) + bias[...][None]
                masked = masked.reshape(height, HD)
                value = masked if n == 1 else jnp.concatenate([masked, value[:, HD:]], axis=1)
            s[:height, :nk] = value

        def soft(g, s, p, al):
            value = s[:height, :nk]
            r = rows(g)
            top = jnp.broadcast_to(jnp.max(value, axis=1, keepdims=True), (height, 128))
            if not first:
                before = m[r]
                top = jnp.maximum(before, top)
                alpha = jnp.exp2((before - top) * SCALE2)
                al[:height] = alpha
            m[r] = top
            shift = top * SCALE2
            part = None
            for j in range(nk // 128):
                e = jnp.exp2(value[:, 128 * j : 128 * j + 128] * SCALE2 - shift)
                p[:height, 128 * j : 128 * j + 128] = e.astype(BF16)
                part = e if part is None else part + e
            l[r] = part if first else l[r] * alpha + part

        def pv(g, p, al):
            r = rows(g)
            values = kv[place : place + n, HD:].reshape(nk, HD)
            new = jnp.dot(p[:height, :nk], values, preferred_element_type=F32)
            if first:
                acc[r] = new
            else:
                alpha = al[:height]
                new = acc[r] * jnp.concatenate([alpha, alpha], axis=1) + new
                if not final:
                    acc[r] = new
                    return
                total = l[r]
                for u in range(group):
                    part = slice(u * TOK, u * TOK + TOK)
                    finish(g * group + u, new[part], total[part])

        qk(0, s_a)
        qk(1, s_b)
        soft(0, s_a, p_a, al_a)

        def body(i, _):
            g = 2 * i + 1
            qk(g + 1, s_a)
            pv(g - 1, p_a, al_a)
            soft(g, s_b, p_b, al_b)
            qk(g + 2, s_b)
            pv(g, p_b, al_b)
            soft(g + 1, s_a, p_a, al_a)
            return 0

        lax.fori_loop(0, count // 2 - 1, body, 0)
        pv(count - 2, p_a, al_a)
        soft(count - 1, s_b, p_b, al_b)
        pv(count - 1, p_b, al_b)

    attend((0,), 4)
    for c in range(CHUNKS):
        for k in range(1, COLS):
            row_copy(c, k).wait_send()
        for to in range(1, ROWS):
            @pl.when(to > z)
            def _():
                col_copy(c, to).wait_send()

    halo.each(halo.first_row)
    for index, step in enumerate(STEPS):
        halo.need(step)

        @pl.when(me >= max(step))
        def _():
            attend(step, 4, final=index == len(STEPS) - 1)

        if len(step) == 2:
            @pl.when((me >= min(step)) & (me < max(step)))
            def _():
                attend((min(step),), 1)

        if index == 0:
            halo.each(halo.second_row)
        if index == 1:
            halo.each(halo.last_row)

    def finish_four(i, _):
        for u in range(PER):
            h = PER * i + u
            r = pl.ds(pl.multiple_of(h * TOK, TOK), TOK)
            finish(h, acc[r], l[r])
        return 0

    @pl.when(me < STEPS[-1][0])
    def _():
        lax.fori_loop(0, CHUNKS, finish_four, 0)

    halo.drain()


def keep(v):
    return pltpu.with_memory_space_constraint(v, pltpu.HBM)


def on_device(inputs, recur_weight, input_weight, recur_bias, input_bias, decay_rate, kv_weight):
    hbm = pl.BlockSpec(memory_space=pltpu.HBM)
    vmem = pl.BlockSpec(memory_space=pltpu.VMEM)
    tile = pltpu.VMEM((TOK, HD), F32)
    dma = pltpu.SemaphoreType.DMA
    return pl.pallas_call(
        kernel,
        in_specs=[hbm] * 7,
        out_specs=vmem,
        out_shape=jax.ShapeDtypeStruct((TOK, D), BF16),
        scratch_shapes=[
            pltpu.VMEM((TOK, D), BF16),
            pltpu.VMEM((HEADS, HD, HD), BF16),
            pltpu.VMEM((HEADS, HD, HD), BF16),
            pltpu.VMEM((1, D), F32),
            pltpu.VMEM((1, D), F32),
            pltpu.VMEM((1, D), F32),
            pltpu.VMEM((HEADS, HD, 2 * HD), BF16),
            pltpu.VMEM((TOK, TOK), BF16),
            pltpu.VMEM((TOK, TOK), BF16),
            tile, tile, tile, tile, tile, tile,
            pltpu.VMEM((HEADS, TOK, HD), F32),
            pltpu.VMEM((HEADS, TOK, HD), F32),
            pltpu.VMEM((HEADS, 8, HD), F32),
            pltpu.VMEM((HEADS, 8, HD), F32),
            pltpu.VMEM((CHUNKS, COLS, 2, PER, 1, HD), F32),
            pltpu.VMEM((CHUNKS, 2, PER, 1, HD), F32),
            pltpu.VMEM((CHUNKS, ROWS, 2, PER, 1, HD), F32),
            pltpu.VMEM((PER, 1, HD), F32),
            pltpu.VMEM((HEADS, TOK, HD), BF16),
            pltpu.VMEM((TOK, 2 * HD), F32),
            pltpu.VMEM((9, 2 * HD, HD), BF16),
            tile, tile,
            pltpu.VMEM((HEADS * TOK, 128), F32),
            pltpu.VMEM((HEADS * TOK, 128), F32),
            pltpu.VMEM((HEADS * TOK, HD), F32),
            pltpu.VMEM((4 * TOK, 2 * HD), F32),
            pltpu.VMEM((4 * TOK, 2 * HD), F32),
            pltpu.VMEM((4 * TOK, 2 * HD), BF16),
            pltpu.VMEM((4 * TOK, 2 * HD), BF16),
            pltpu.VMEM((4 * TOK, 128), F32),
            pltpu.VMEM((4 * TOK, 128), F32),
            dma((3 * CHUNKS + 4,)),
            dma((CHUNKS, COLS - 1)),
            dma((CHUNKS, COLS)),
            dma((CHUNKS, ROWS)),
            dma((CHUNKS, ROWS)),
            dma((17 * PARTS // 2,)),
            dma((9, PARTS)),
        ],
        compiler_params=pltpu.CompilerParams(
            collective_id=0, has_side_effects=True, vmem_limit_bytes=51 * 1024 * 1024
        ),
        name="layer",
    )(
        inputs, recur_weight, input_weight, keep(recur_bias[None]), keep(input_bias[None]),
        keep(decay_rate[None]), kv_weight.reshape(HEADS, HD, 2 * HD),
    )


def solution(mesh):
    placed = (P(("batch", "seq"), None), P(), P(), P(), P(), P(), P())
    return jax.shard_map(
        on_device, mesh=mesh, in_specs=placed, out_specs=P(("batch", "seq"), None), check_vma=False
    )
```
